32 devices in a mesh: dp: 1 (over z), m1: 4 (over y), m2: 8 (over x, core).
Axes of the slice: x: 4, y: 4, z: 1, core: 2. Of those that a mesh axis runs over, the one named last changes fastest.
The devices are a block of a 4x4x8 slice.
Arguments:
- x: bfloat16 [32, 256, 4096], P('dp', None, 'm1')
- ln_scale: float32 [4096], replicated
- qn_scale: float32 [128], replicated
- kn_scale: float32 [128], replicated
- w_qkv: bfloat16 [4096, 3, 4096], P('m1', None, 'm2')
- w_up: bfloat16 [4096, 16384], P('m1', 'm2')
- b_up: float32 [16384], P('m2')
- w_o: bfloat16 [4096, 4096], P('m2', 'm1')
- w_down: bfloat16 [16384, 4096], P('m2', 'm1')
- b_out: float32 [4096], P('m1')
Outputs:
- output: bfloat16 [32, 256, 4096], P('dp', None, 'm1')
All inputs are finite; a program needn't handle non-finite values.
Results may differ from the reference program's by a relative error of at most 0.0111303.
Values are sent between devices in bfloat16 or wider.
A program may use at most 768 MiB of HBM per device.

```python
import jax
import jax.numpy as jnp
from jax import lax

BATCH = 32
PATCHES = 256
MODEL_DIM = 4096
HEADS = 32
HEAD_DIM = 128
MLP_DIM = 16384
LN_EPS = 1e-6


def setup_inputs(seed: int = 0, part: int = 0) -> dict:
    part_key = jax.random.fold_in(jax.random.key(seed), part)
    key_mean, key_scale, key_noise = jax.random.split(part_key, 3)
    shared = jax.random.split(jax.random.key(seed + 1), 9)
    qkv_width = HEADS * HEAD_DIM
    tok_mean = 1.5 * jax.random.normal(key_mean, (BATCH, PATCHES, 1), jnp.float32)
    tok_scale = jax.random.uniform(key_scale, (BATCH, PATCHES, 1), jnp.float32, 0.5, 2.0)
    col_scale = 0.5 + 1.5 * jnp.arange(MODEL_DIM, dtype=jnp.float32) / MODEL_DIM
    noise = jax.random.normal(key_noise, (BATCH, PATCHES, MODEL_DIM), jnp.float32)
    x = (tok_mean + tok_scale * col_scale * noise).astype(jnp.bfloat16)
    ln_scale = jax.random.uniform(shared[0], (MODEL_DIM,), jnp.float32, 0.5, 1.5)
    qn_scale = jax.random.uniform(shared[1], (HEAD_DIM,), jnp.float32, 1.0, 2.5)
    kn_scale = jax.random.uniform(shared[2], (HEAD_DIM,), jnp.float32, 1.0, 2.5)
    w_qkv = (jax.random.normal(shared[3], (MODEL_DIM, 3, qkv_width), jnp.float32) * MODEL_DIM ** -0.5).astype(jnp.bfloat16)
    w_up = (jax.random.normal(shared[4], (MODEL_DIM, MLP_DIM), jnp.float32) * MODEL_DIM ** -0.5).astype(jnp.bfloat16)
    b_up = 0.5 * jax.random.normal(shared[5], (MLP_DIM,), jnp.float32)
    w_o = (jax.random.normal(shared[6], (qkv_width, MODEL_DIM), jnp.float32) * qkv_width ** -0.5).astype(jnp.bfloat16)
    w_down = (jax.random.normal(shared[7], (MLP_DIM, MODEL_DIM), jnp.float32) * MLP_DIM ** -0.5).astype(jnp.bfloat16)
    b_out = 0.5 * jax.random.normal(shared[8], (MODEL_DIM,), jnp.float32)
    return {'x': x, 'ln_scale': ln_scale, 'qn_scale': qn_scale, 'kn_scale': kn_scale, 'w_qkv': w_qkv, 'w_up': w_up, 'b_up': b_up, 'w_o': w_o, 'w_down': w_down, 'b_out': b_out}


def layer_norm(values, scale):
    mean = jnp.mean(values, axis=-1, keepdims=True)
    centered = values - mean
    variance = jnp.mean(centered * centered, axis=-1, keepdims=True)
    return centered * lax.rsqrt(variance + LN_EPS) * scale


def attend_one(operands):
    queries, keys, values = operands
    scores = jnp.einsum('nhd,mhd->hnm', queries.astype(jnp.float32), keys.astype(jnp.float32)) * HEAD_DIM ** -0.5
    attn_probs = jax.nn.softmax(scores, axis=-1).astype(jnp.bfloat16)
    attended = jnp.einsum('hnm,mhd->nhd', attn_probs.astype(jnp.float32), values.astype(jnp.float32))
    return attended.astype(jnp.bfloat16)


def reference(x, ln_scale, qn_scale, kn_scale, w_qkv, w_up, b_up, w_o, w_down, b_out):
    tokens = BATCH * PATCHES
    qkv_width = HEADS * HEAD_DIM
    x_flat = x.reshape(tokens, MODEL_DIM).astype(jnp.float32)
    normed = layer_norm(x_flat, ln_scale).astype(jnp.bfloat16)
    proj_qkv = jnp.dot(normed, w_qkv.reshape(MODEL_DIM, 3 * qkv_width), preferred_element_type=jnp.float32).astype(jnp.bfloat16)
    proj_qkv = proj_qkv.reshape(BATCH, PATCHES, 3, HEADS, HEAD_DIM)
    queries = layer_norm(proj_qkv[:, :, 0].astype(jnp.float32), qn_scale).astype(jnp.bfloat16)
    keys = layer_norm(proj_qkv[:, :, 1].astype(jnp.float32), kn_scale).astype(jnp.bfloat16)
    attended = lax.map(attend_one, (queries, keys, proj_qkv[:, :, 2]))
    up_in = jnp.dot(normed, w_up, preferred_element_type=jnp.float32).astype(jnp.bfloat16)
    hidden = jax.nn.gelu(up_in.astype(jnp.float32) + b_up, approximate=False).astype(jnp.bfloat16)
    mixed_sum = jnp.dot(attended.reshape(tokens, qkv_width), w_o, preferred_element_type=jnp.float32) + jnp.dot(hidden, w_down, preferred_element_type=jnp.float32)
    result = x_flat + mixed_sum + b_out
    return result.astype(jnp.bfloat16).reshape(BATCH, PATCHES, MODEL_DIM)
```

```python
import functools

import jax
import jax.numpy as jnp
from jax import lax
from jax.experimental import pallas as pl
from jax.experimental.pallas import tpu as pltpu
from jax.sharding import PartitionSpec as P

LN_EPS = 1e-6
CORES = 2
VMEM_MAX = 67043328
MESH = pl.DeviceIdType.MESH


def layer_norm(values, scale):
    mean = jnp.mean(values, axis=-1, keepdims=True)
    centered = values - mean
    variance = jnp.mean(centered * centered, axis=-1, keepdims=True)
    return centered * lax.rsqrt(variance + LN_EPS) * scale


def out_kernel(rows, chips, seq, h_hbm, w_own, w_near_b, w_near_t, x_hbm, bias, out_hbm, h_v, w_v, d_v, rd_v, x_v, rx_v, half_v, tot_v, rh_v,
               fin_v, fa_v, loc_sem, w_send, w_recv, d_send, d_recv, x_send, x_recv, y_send, y_recv, g_send, g_recv, s_send, s_recv):
    dp, row, col = lax.axis_index('dp'), lax.axis_index('m1'), lax.axis_index('m2')
    chip, core = col // CORES, lax.rem(col, CORES)
    patches = x_hbm.shape[1]
    images = h_v.shape[0] // patches
    hk = w_own.shape[0] // 2
    hp = patches // 2

    def peer(dy=0, dx=0, dc=0):
        return (dp, lax.rem(row + dy, rows), lax.rem(chip + dx, chips) * CORES + lax.rem(core + dc, CORES))

    def remote(src, dst, ssem, rsem, who):
        return pltpu.make_async_remote_copy(src_ref=src, dst_ref=dst, send_sem=ssem, recv_sem=rsem, device_id=who, device_id_type=MESH)

    barrier = pltpu.get_barrier_semaphore()
    partners = [peer(dy=d) for d in range(1, rows)] + [peer(dx=1), peer(dx=chips - 1), peer(dc=1)]
    for who in partners:
        pl.semaphore_signal(barrier, inc=1, device_id=who, device_id_type=MESH)
    pl.semaphore_wait(barrier, len(partners))

    top, bot = pl.ds(0, hk), pl.ds(hk, hk)
    w_copies = [
        remote(w_own.at[bot, :], w_v.at[3, bot, :], w_send.at[0], w_recv.at[0], peer(dy=1)),
        remote(w_own.at[top, :], w_v.at[1, top, :], w_send.at[1], w_recv.at[1], peer(dy=rows - 1)),
        remote(w_near_t, w_v.at[2, top, :], w_send.at[2], w_recv.at[2], peer(dy=1)),
        remote(w_near_b, w_v.at[2, bot, :], w_send.at[3], w_recv.at[3], peer(dy=rows - 1)),
    ]
    for c in w_copies:
        c.start()
    h_copy = pltpu.make_async_copy(h_hbm, h_v, loc_sem.at[0])
    own_copy = pltpu.make_async_copy(w_own, w_v.at[0], loc_sem.at[1])
    nb_copy = pltpu.make_async_copy(w_near_b, w_v.at[1, bot, :], loc_sem.at[2])
    nt_copy = pltpu.make_async_copy(w_near_t, w_v.at[3, top, :], loc_sem.at[3])
    h_copy.start()
    own_copy.start()
    nb_copy.start()
    nt_copy.start()

    def home_image(r):
        return lax.rem(row - r + rows, rows) * images + col

    res_copies = [pltpu.make_async_copy(x_hbm.at[home_image(r)], fin_v.at[q], loc_sem.at[4 + q]) for q, r in enumerate(seq)]
    for c in res_copies:
        c.start()
    h_copy.wait()

    def dot(t, r):
        lhs = h_v[pl.ds(pl.multiple_of(t * patches, patches), patches), :]
        return jnp.dot(lhs, w_v[r], preferred_element_type=jnp.float32).astype(jnp.bfloat16)

    def d_copy(q, dx):
        return remote(d_v.at[q % 2, dx], rd_v.at[q % 2, dx], d_send.at[q, dx], d_recv.at[q, dx], peer(dc=1))

    def x_copy(q, k):
        s = q % 2
        src = [x_v.at[s, 1], x_v.at[s, chips - 1], x_v.at[s, 2, pl.ds(0, hp), :], x_v.at[s, 2, pl.ds(hp, hp), :]][k]
        dst = rx_v.at[q, k] if k < 2 else half_v.at[q, k - 2]
        return remote(src, dst, x_send.at[q, k], x_recv.at[q, k], peer(dx=1 if k % 2 == 0 else chips - 1))

    def y_copy(q, r):
        return remote(tot_v.at[q], rh_v.at[q], y_send.at[q], y_recv.at[q], peer(dy=r))

    def image_of(r, dx, dc=0):
        return lax.rem(row - r + rows, rows) * images + lax.rem(chip + dx, chips) * CORES + lax.rem(core + dc, CORES)

    def g_copy(q, r, k):
        if k < 2:
            src, dst = fin_v.at[q], fa_v.at[q, k]
        else:
            part = pl.ds((k - 2) * hp, hp)
            src, dst = fa_v.at[q, k - 2, part, :], fa_v.at[q, 2, part, :]
        return remote(src, dst, g_send.at[q, k], g_recv.at[q, k], peer(dx=1 if k % 2 == 0 else chips - 1))

    def s_copy(q, r, k):
        src = fin_v.at[q] if k == 0 else fa_v.at[q, k - 1]
        image = image_of(r, [0, chips - 1, 1, 2][k])
        return remote(src, out_hbm.at[image], s_send.at[q, k], s_recv.at[q, k], peer(dc=1))

    def l_copy(q, r, k):
        src = fin_v.at[q] if k == 0 else fa_v.at[q, k - 1]
        image = image_of(r, [0, chips - 1, 1, 2][k])
        return pltpu.make_async_copy(src, out_hbm.at[image], loc_sem.at[8 + q * 4 + k])

    def spread(q, r, k):
        s_copy(q, r, k).start()
        l_copy(q, r, k).start()

    def compute(q, r):
        s = q % 2
        if q >= 2:
            for dx in range(chips):
                d_copy(q - 2, dx).wait_send()
            for k in range(4):
                x_copy(q - 2, k).wait_send()

        def sibling(dx, carry):
            d_v[s, dx] = dot(chips + dx, r)
            d_copy(q, dx).start()
            return carry

        lax.fori_loop(0, chips, sibling, 0)

        def own(k, carry):
            dx = lax.rem(k + 2, chips)
            part = dot(dx, r).astype(jnp.float32)
            d_copy(q, dx).wait_recv()
            x_v[s, dx] = (part + rd_v[s, dx].astype(jnp.float32)).astype(jnp.bfloat16)

            @pl.when(k == 0)
            def _():
                x_copy(q, 2).start()
                x_copy(q, 3).start()

            return carry

        lax.fori_loop(0, chips, own, 0)

    def mid(q, r):
        s = q % 2
        for k, (dx, part) in enumerate(((1, pl.ds(0, hp)), (chips - 1, pl.ds(hp, hp)))):
            x_copy(q, 2 + k).wait_recv()
            x_v[s, dx, part, :] = (x_v[s, dx, part, :].astype(jnp.float32) + half_v[q, k].astype(jnp.float32)).astype(jnp.bfloat16)
            x_copy(q, k).start()

    def reduce(q, r):
        x_copy(q, 0).wait_recv()
        x_copy(q, 1).wait_recv()
        tot_v[q] = (x_v[q % 2, 0].astype(jnp.float32) + rx_v[q, 0].astype(jnp.float32) + rx_v[q, 1].astype(jnp.float32)).astype(jnp.bfloat16)
        if r:
            y_copy(q, r).start()

    def home(q, r):
        if r:
            y_copy(q, r).wait_recv()
        total = (rh_v if r else tot_v)[q].astype(jnp.float32)
        res_copies[q].wait()
        fin_v[q] = (fin_v[q].astype(jnp.float32) + total + bias[...]).astype(jnp.bfloat16)
        g_copy(q, r, 0).start()
        g_copy(q, r, 1).start()
        spread(q, r, 0)

    def near(q, r):
        for k in range(2):
            g_copy(q, r, k).wait_recv()
            g_copy(q, r, 2 + k).start()
            spread(q, r, 1 + k)

    def far(q, r):
        g_copy(q, r, 2).wait_recv()
        g_copy(q, r, 3).wait_recv()
        spread(q, r, 3)

    own_copy.wait()
    for step in (compute, mid, reduce, home, near, far):
        step(0, seq[0])
    nb_copy.wait()
    w_copies[1].wait_recv()
    compute(1, seq[1])
    nt_copy.wait()
    w_copies[0].wait_recv()
    mid(1, seq[1])
    compute(2, seq[2])
    mid(2, seq[2])
    for step in (reduce, home):
        step(1, seq[1])
        step(2, seq[2])
    w_copies[2].wait_recv()
    w_copies[3].wait_recv()
    compute(3, seq[3])
    near(1, seq[1])
    near(2, seq[2])
    mid(3, seq[3])
    far(1, seq[1])
    far(2, seq[2])
    for step in (reduce, home, near, far):
        step(3, seq[3])
    for q, r in enumerate(seq):
        for k in range(4):
            s_copy(q, r, k).wait_recv()
            s_copy(q, r, k).wait_send()
            l_copy(q, r, k).wait()
            g_copy(q, r, k).wait_send()
        if r:
            y_copy(q, r).wait_send()
    for q in (2, 3):
        for k in range(4):
            d_copy(q, k).wait_send()
            x_copy(q, k).wait_send()
    for c in w_copies:
        c.wait_send()


def out_layer(rows, chips, h, w_own, w_near_b, w_near_t, x_blk, b_out):
    batch, patches, dim_local = x_blk.shape
    seq = (0, 1, 3, 2)
    bf, vm = jnp.bfloat16, pltpu.VMEM
    piece = (patches, dim_local)
    anyspec = pl.BlockSpec(memory_space=pl.ANY)
    return pl.pallas_call(
        functools.partial(out_kernel, rows, chips, seq),
        out_shape=jax.ShapeDtypeStruct(x_blk.shape, bf),
        in_specs=[anyspec] * 5 + [pl.BlockSpec(memory_space=pltpu.VMEM)],
        out_specs=anyspec,
        scratch_shapes=[
            vm(h.shape, bf), vm((rows,) + w_own.shape, bf), vm((2, chips) + piece, bf), vm((2, chips) + piece, bf), vm((2, chips) + piece, bf),
            vm((rows, 2) + piece, bf), vm((rows, 2, patches // 2, dim_local), bf), vm((rows,) + piece, bf), vm((rows,) + piece, bf), vm((rows,) + piece, bf),
            vm((rows, 3) + piece, bf),
            pltpu.SemaphoreType.DMA((24,)),
            pltpu.SemaphoreType.DMA((4,)), pltpu.SemaphoreType.DMA((4,)),
        ] + [pltpu.SemaphoreType.DMA((rows, 4))] * 4 + [pltpu.SemaphoreType.DMA((rows,))] * 2 + [pltpu.SemaphoreType.DMA((rows, 4))] * 4,
        compiler_params=pltpu.CompilerParams(collective_id=0, has_side_effects=True, vmem_limit_bytes=VMEM_MAX),
        cost_estimate=pl.CostEstimate(flops=2 * h.shape[0] * h.shape[1] * dim_local * rows, bytes_accessed=1 << 27, transcendentals=0),
        name='out_layer',
    )(h, w_own, w_near_b, w_near_t, x_blk, b_out.reshape(1, dim_local))


def solution(mesh):
    rows = mesh.shape['m1']
    cols = mesh.shape['m2']
    chips = cols // CORES
    assert rows == 4 and chips == 4

    def hop(value, dy, dx=0, dc=0):
        pairs = []
        for y in range(rows):
            for c in range(cols):
                chip, core = divmod(c, CORES)
                target = ((y + dy) % rows) * cols + ((chip + dx) % chips) * CORES + (core + dc) % CORES
                pairs.append((y * cols + c, target))
        return lax.ppermute(value, ('m1', 'm2'), pairs)

    def after(value, *others):
        return lax.optimization_barrier((value,) + others)[0]

    def local_layer(x_blk, ln_scale, qn_scale, kn_scale, w_qkv, w_up, b_up, w_o, w_down, b_out):
        batch, patches, dim_local = x_blk.shape
        head_dim = qn_scale.shape[0]
        heads_local = w_qkv.shape[2] // head_dim
        row, col = lax.axis_index('m1'), lax.axis_index('m2')
        chip, core = col // CORES, col % CORES
        per_row = batch // rows

        pieces = [None] * rows
        for d in range(rows):
            image = lax.rem(row + d, rows) * per_row + col
            piece = lax.dynamic_slice_in_dim(x_blk, image, 1, 0)
            pieces[-d % rows] = piece if d == 0 else hop(piece, d)
        scale_rel = [lax.dynamic_slice_in_dim(ln_scale, lax.rem(row + r, rows) * dim_local, dim_local) for r in range(rows)]
        image_x = jnp.concatenate(pieces, axis=-1).astype(jnp.float32)
        u_own = layer_norm(image_x, jnp.concatenate(scale_rel)).astype(jnp.bfloat16)

        def gather_cols(own):
            near = [own, hop(own, 0, -1), hop(own, 0, -2), hop(own, 0, -3)]
            far = [hop(v, 0, 0, 1) for v in near]
            return near, far

        near, far = gather_cols(u_own)
        u = jnp.concatenate(near + far, axis=0).reshape(per_row * patches, rows * dim_local)

        def gather_rows(top, bottom, gate=None):
            if gate is not None:
                top, bottom = lax.optimization_barrier((top, bottom, gate))[:2]
            t3, b1 = hop(top, 1), hop(bottom, -1)
            b3, t1 = hop(bottom, 1), hop(top, -1)
            t2, b2 = hop(t3, 1), hop(b1, -1)
            return [(top, bottom), (t1, b1), (t2, b2), (t3, b3)]

        half = dim_local // 2
        qkv_w = w_qkv.reshape(dim_local, -1)
        n_up = w_up.shape[1] // 2
        g_qkv = gather_rows(qkv_w[:half], qkv_w[half:])
        g_up0 = gather_rows(w_up[:half, :n_up], w_up[half:, :n_up], g_qkv[3][0])
        g_up1 = gather_rows(w_up[:half, n_up:], w_up[half:, n_up:], g_up0[3][0])
        w2 = jnp.concatenate([w_o, w_down], axis=0)
        k_half = w2.shape[0] // 2
        w2_top, w2_bot = lax.optimization_barrier((w2[:k_half], w2[k_half:], g_up1[3][0]))[:2]
        near_t, near_b = hop(w2_top, 1), hop(w2_bot, -1)

        def project(parts):
            weight = jnp.concatenate([v for pair in parts for v in pair], axis=0)
            return jnp.dot(u, weight, preferred_element_type=jnp.float32).astype(jnp.bfloat16)

        qkv = project(g_qkv).reshape(per_row, patches, 3, heads_local, head_dim)
        queries = layer_norm(qkv[:, :, 0].astype(jnp.float32), qn_scale).astype(jnp.bfloat16)
        keys = layer_norm(qkv[:, :, 1].astype(jnp.float32), kn_scale).astype(jnp.bfloat16)
        scores = jnp.einsum('bnhd,bmhd->bhnm', queries, keys, preferred_element_type=jnp.float32) * head_dim ** -0.5
        probs = jax.nn.softmax(scores, axis=-1).astype(jnp.bfloat16)
        attended = jnp.einsum('bhnm,bmhd->bnhd', probs, qkv[:, :, 2], preferred_element_type=jnp.float32).astype(jnp.bfloat16)
        attended = attended.reshape(per_row * patches, heads_local * head_dim)

        def act(parts, bias):
            up_in = project(parts).astype(jnp.float32)
            return jax.nn.gelu(up_in + bias, approximate=False).astype(jnp.bfloat16)

        hidden = [act(g_up0, b_up[:n_up]), act(g_up1, b_up[n_up:])]
        h = jnp.concatenate([attended] + hidden, axis=1)

        return out_layer(rows, chips, h, w2, near_b, near_t, x_blk, b_out)

    return jax.shard_map(local_layer, mesh=mesh, in_specs=(P('dp', None, 'm1'), P(), P(), P(), P('m1', None, 'm2'), P('m1', 'm2'), P('m2'), P('m2', 'm1'), P('m2', 'm1'), P('m1')), out_specs=P('dp', None, 'm1'), check_vma=False)
```

```python
import functools

import jax
import jax.numpy as jnp
from jax import lax
from jax.experimental import pallas as pl
from jax.experimental.pallas import tpu as pltpu
from jax.sharding import PartitionSpec as P

LN_EPS = 1e-6
CORES = 2
LINES = 16
VMEM_MAX = 67043328
MESH = pl.DeviceIdType.MESH


def layer_norm(values, scale):
    mean = jnp.mean(values, axis=-1, keepdims=True)
    centered = values - mean
    variance = jnp.mean(centered * centered, axis=-1, keepdims=True)
    return centered * lax.rsqrt(variance + LN_EPS) * scale


class Place:
    def __init__(self, rows, chips):
        self.rows, self.chips = rows, chips
        self.dp, self.row = lax.axis_index('dp'), lax.axis_index('m1')
        col = lax.axis_index('m2')
        self.col, self.chip, self.core = col, col // CORES, lax.rem(col, CORES)
        self.inner = self.row + 1 - 2 * lax.rem(self.row, 2)
        self.cross = rows - 1 - self.row
        self.pair = self.row // 2
        self.half = lax.rem((self.row + 1) // 2, 2)
        self.primary = self.core == self.pair
        self.inner_peer = (self.dp, self.inner, col)
        self.cross_peer = (self.dp, self.cross, col)
        self.right_peer = (self.dp, self.row, self.at(1) * CORES + self.core)
        self.left_peer = (self.dp, self.row, self.at(chips - 1) * CORES + self.core)
        self.sibling = (self.dp, self.row, self.chip * CORES + 1 - self.core)

    def at(self, dx):
        return lax.rem(self.chip + dx, self.chips)

    def enter(self):
        barrier = pltpu.get_barrier_semaphore()
        partners = (self.inner_peer, self.cross_peer, self.right_peer, self.left_peer, self.sibling)
        for who in partners:
            pl.semaphore_signal(barrier, inc=1, device_id=who, device_id_type=MESH)
        pl.semaphore_wait(barrier, len(partners))

    def first_image(self, half, dx, core, batch):
        per = batch // (2 * CORES)
        return (half * CORES + core) * per + self.at(dx) * (per // self.chips)


def remote(src, dst, ssem, rsem, who):
    return pltpu.make_async_remote_copy(src_ref=src, dst_ref=dst, send_sem=ssem, recv_sem=rsem, device_id=who, device_id_type=MESH)


def aligned(index, size):
    return pl.ds(pl.multiple_of(index * size, size), size)


def stage_one_kernel(rows, chips, heads, x_hbm, ln_scale, qk_scale, bias_own, wq, wu, h_hbm, raw, u_v, w_v, qkv_v, st_v, up_v, at_v, bias_v,
                     xs_send, xs_recv, ag_send, ag_recv, ld_sem, own_sem, b_send, b_recv, wa_send, wa_recv, wb_send, wb_recv, wc_send, wc_recv,
                     wd_send, wd_recv, up_sem, at_sem):
    p = Place(rows, chips)
    batch, patches, dim_local = x_hbm.shape
    dim = dim_local * rows
    wide = wq.shape[2]
    head_dim = wide // heads
    n_q, n_up = wq.shape[0], wu.shape[1] // wide
    n_w = n_q + n_up
    sub = batch // (2 * CORES * chips)
    group = sub * patches
    dx_of = (0, chips - 1, 1, 2)

    xa = remote(x_hbm.at[pl.ds(p.first_image(p.half, 0, p.core, batch), sub)], raw.at[0, 1], xs_send.at[0], xs_recv.at[0], p.cross_peer)
    xb = remote(x_hbm.at[pl.ds(p.first_image(1 - p.half, 0, p.core, batch), sub)], raw.at[0, 0], xs_send.at[1], xs_recv.at[1], p.inner_peer)
    xc = remote(raw.at[0, 0], raw.at[0, 2], xs_send.at[2], xs_recv.at[2], p.cross_peer)

    def ag(e, k):
        src, dst = ((raw.at[0, e], raw.at[1, e]), (raw.at[0, e], raw.at[2, e]), (raw.at[1, e, 0], raw.at[3, e, 0]), (raw.at[2, e, 1], raw.at[3, e, 1]))[k]
        return remote(src, dst, ag_send.at[e, k], ag_recv.at[e, k], p.right_peer if k % 2 == 0 else p.left_peer)

    def block(r, k):
        return w_v.at[pl.ds(r * dim_local, dim_local), aligned(k, wide)]

    def from_own(k, make, act):
        @pl.when(k < n_q)
        def _():
            act(make(wq.at[jnp.minimum(k, n_q - 1)]))

        @pl.when(k >= n_q)
        def _():
            act(make(wu.at[:, aligned(jnp.maximum(k - n_q, 0), wide)]))

    def wa(k, src=None):
        return remote(block(1, k) if src is None else src, block(1, k), wa_send.at[k], wa_recv.at[k], p.inner_peer)

    def wb(k, src=None):
        return remote(block(2, k) if src is None else src, block(2, k), wb_send.at[k], wb_recv.at[k], p.cross_peer)

    def wc(k):
        return remote(block(2, k), block(3, k), wc_send.at[k], wc_recv.at[k], p.inner_peer)

    def wd(r, k, src=None):
        return remote(block(r, k) if src is None else src, block(r, k), wd_send.at[r, k], wd_recv.at[r, k], p.sibling)

    own_copies = [pltpu.make_async_copy(wq.at[k], block(0, k), own_sem.at[k]) for k in range(n_q)]
    own_copies.append(pltpu.make_async_copy(wu, w_v.at[pl.ds(0, dim_local), pl.ds(n_q * wide, n_up * wide)], own_sem.at[n_q]))
    bias_copy = remote(bias_own, bias_v, b_send, b_recv, p.sibling)

    def start(copy):
        copy.start()

    def pump(k):
        @pl.when(p.primary)
        def _():
            wb(k).wait_recv()
            wc(k).start()
            wd(2, k).start()
            wa(k).wait_recv()
            wd(1, k).start()
            if k + 2 < n_w:
                from_own(k + 2, functools.partial(wa, k + 2), start)
                from_own(k + 2, functools.partial(wd, 0, k + 2), start)

    def finish(k):
        @pl.when(p.primary)
        def _():
            wc(k).wait_recv()
            wd(3, k).start()

        @pl.when(jnp.logical_not(p.primary))
        def _():
            for r in range(rows):
                wd(r, k).wait_recv()

    def load_copies(rank_dx, rank, s, b):
        image = p.first_image(p.half, rank_dx, p.core, batch) + s
        yield pltpu.make_async_copy(x_hbm.at[image], st_v.at[b, :, pl.ds(0, dim_local)], ld_sem.at[b, 0])
        for e in range(rows - 1):
            yield pltpu.make_async_copy(raw.at[rank, e, s], st_v.at[b, :, pl.ds((e + 1) * dim_local, dim_local)], ld_sem.at[b, e + 1])

    def normalize(ranks):
        jobs = [(rank, s) for rank in ranks for s in range(sub)]
        loads = [list(load_copies(dx_of[rank], rank, s, n % 2)) for n, (rank, s) in enumerate(jobs)]
        for n in range(len(jobs)):
            if n == 0:
                for c in loads[0]:
                    c.start()
            if n + 1 < len(jobs):
                for c in loads[n + 1]:
                    c.start()
            for c in loads[n]:
                c.wait()
            rank, s = jobs[n]

            def lines(m, carry, b=n % 2, base=(rank * sub + s) * patches):
                here = aligned(m, LINES)
                wide_x = st_v[b, here, :].astype(jnp.float32)
                to = pl.ds(pl.multiple_of(base + m * LINES, LINES), LINES)
                u_v[to, :] = layer_norm(wide_x, ln_scale[...]).astype(jnp.bfloat16)
                return carry

            lax.fori_loop(0, patches // LINES, lines, 0)

    def dot_cell(rank, k):
        return jnp.dot(u_v[aligned(rank, group), :], w_v[:, aligned(k, wide)], preferred_element_type=jnp.float32).astype(jnp.bfloat16)

    def qkv_cell(rank, k):
        z = dot_cell(rank, k)
        to = aligned(rank, group)

        @pl.when(k == n_q - 1)
        def _():
            qkv_v[k, to, :] = z

        @pl.when(k < n_q - 1)
        def _():
            scale = qk_scale[pl.ds(k, 1), :]
            for hd in range(heads):
                part = slice(hd * head_dim, (hd + 1) * head_dim)
                qkv_v[k, to, part] = layer_norm(z[:, part].astype(jnp.float32), scale).astype(jnp.bfloat16)

    def at_copy(image, b):
        return pltpu.make_async_copy(at_v.at[b], h_hbm.at[aligned(image, patches), pl.ds(0, wide)], at_sem.at[b])

    def attend(first, count):
        def one(image, carry):
            b = lax.rem(image, 2)
            here = aligned(image, patches)

            @pl.when(image >= 2)
            def _():
                at_copy(image - 2, b).wait()

            for hd in range(heads):
                part = slice(hd * head_dim, (hd + 1) * head_dim)
                q, k, v = (qkv_v[n, here, part] for n in range(3))
                scores = lax.dot_general(q, k, (((1,), (1,)), ((), ())), preferred_element_type=jnp.float32) * head_dim ** -0.5
                probs = jnp.exp(scores - jnp.max(scores, axis=-1, keepdims=True))
                probs = (probs / jnp.sum(probs, axis=-1, keepdims=True)).astype(jnp.bfloat16)
                at_v[b, :, part] = jnp.dot(probs, v, preferred_element_type=jnp.float32).astype(jnp.bfloat16)
            at_copy(image, b).start()
            return carry

        lax.fori_loop(first, first + count, one, 0)

    def up_copy(rank, k, b):
        return pltpu.make_async_copy(up_v.at[b], h_hbm.at[aligned(rank, group), aligned(k - n_q + 1, wide)], up_sem.at[b])

    def up_chunk(k, carry):
        finish(k)
        here = aligned(k - n_q, wide)
        bias = jnp.where(p.primary, bias_own[:, here], bias_v[:, here])

        def cell(rank, carry):
            b = lax.rem(rank, 2)

            @pl.when(jnp.logical_or(k > n_q, rank >= 2))
            def _():
                up_copy(rank, k, b).wait()

            m = dot_cell(rank, k).astype(jnp.float32) + bias
            up_v[b] = (0.5 * m * (1.0 + lax.erf(m * 0.5 ** 0.5))).astype(jnp.bfloat16)
            up_copy(rank, k, b).start()
            return carry

        return lax.fori_loop(0, rows, cell, carry)

    p.enter()
    xb.start()
    xa.start()
    bias_copy.start()

    @pl.when(p.primary)
    def _():
        for c in own_copies:
            c.start()
        for k in (0, 1):
            from_own(k, functools.partial(wa, k), start)
            from_own(k, functools.partial(wd, 0, k), start)

    @pl.when(jnp.logical_not(p.primary))
    def _():
        from_own(0, functools.partial(wb, 0), start)

    xb.wait_recv()
    xc.start()
    ag(0, 0).start()
    ag(0, 1).start()

    @pl.when(jnp.logical_not(p.primary))
    def _():
        for k in range(1, n_w):
            from_own(k, functools.partial(wb, k), start)

    xa.wait_recv()
    ag(1, 0).start()
    ag(1, 1).start()
    pump(0)
    xc.wait_recv()
    ag(2, 0).start()
    ag(2, 1).start()
    pump(1)
    normalize((0,))
    for e in range(rows - 1):
        for k in range(2):
            ag(e, k).wait_recv()
            ag(e, 2 + k).start()
        if e == 0:
            pump(2)
    pump(3)
    normalize((1, 2))

    @pl.when(p.primary)
    def _():
        for c in own_copies:
            c.wait()

    def first_ranks(k, carry):
        finish(k)

        @pl.when(k == 1)
        def _():
            pump(4)

        def cell(rank, carry):
            qkv_cell(rank, k)
            return carry

        return lax.fori_loop(0, rows - 1, cell, carry)

    lax.fori_loop(0, n_q, first_ranks, 0)
    attend(0, (rows - 1) * sub)
    pump(5)
    for e in range(rows - 1):
        ag(e, 2).wait_recv()
        ag(e, 3).wait_recv()
    normalize((rows - 1,))

    def last_rank(k, carry):
        qkv_cell(rows - 1, k)
        return carry

    lax.fori_loop(0, n_q, last_rank, 0)
    pump(6)
    attend((rows - 1) * sub, sub)
    bias_copy.wait_recv()
    lax.fori_loop(n_q, n_w, up_chunk, 0)

    for b in range(2):
        at_copy(b, b).wait()
        up_copy(b, n_q, b).wait()
    for c in (xa, xb, xc, bias_copy):
        c.wait_send()
    for e in range(rows - 1):
        for k in range(4):
            ag(e, k).wait_send()

    @pl.when(p.primary)
    def _():
        for k in range(n_w):
            wa(k).wait_send()
            wc(k).wait_send()
            for r in range(rows):
                wd(r, k).wait_send()

    @pl.when(jnp.logical_not(p.primary))
    def _():
        for k in range(n_w):
            wb(k).wait_send()


def stage_one(rows, chips, x_blk, ln_scale, qk_scale, b_up, wq, wu):
    batch, patches, dim_local = x_blk.shape
    dim, wide = rows * dim_local, wq.shape[2]
    heads = wide // qk_scale.shape[1]
    n_q, n_up = wq.shape[0], wu.shape[1] // wide
    n_w = n_q + n_up
    sub = batch // (2 * CORES * chips)
    tokens = chips * sub * patches
    bf, vm, dma = jnp.bfloat16, pltpu.VMEM, pltpu.SemaphoreType.DMA
    anyspec, vmspec = pl.BlockSpec(memory_space=pl.ANY), pl.BlockSpec(memory_space=pltpu.VMEM)
    h, _ = pl.pallas_call(
        functools.partial(stage_one_kernel, rows, chips, heads),
        out_shape=(jax.ShapeDtypeStruct((tokens, wide + n_up * wide), bf), jax.ShapeDtypeStruct((chips, rows - 1, sub, patches, dim_local), bf)),
        in_specs=[anyspec, vmspec, vmspec, vmspec, anyspec, anyspec],
        out_specs=(anyspec, anyspec),
        scratch_shapes=[
            vm((tokens, dim), bf), vm((dim, n_w * wide), bf), vm((n_q, tokens, wide), bf), vm((2, patches, dim), bf),
            vm((2, sub * patches, wide), bf), vm((2, patches, wide), bf), vm(b_up.shape, jnp.float32),
            dma((3,)), dma((3,)), dma((rows - 1, 4)), dma((rows - 1, 4)), dma((2, rows)), dma((n_q + 1,)), dma, dma,
            dma((n_w,)), dma((n_w,)), dma((n_w,)), dma((n_w,)), dma((n_w,)), dma((n_w,)), dma((rows, n_w)), dma((rows, n_w)), dma((2,)), dma((2,)),
        ],
        compiler_params=pltpu.CompilerParams(collective_id=0, has_side_effects=True, vmem_limit_bytes=VMEM_MAX),
        cost_estimate=pl.CostEstimate(flops=2 * tokens * dim * n_w * wide, bytes_accessed=1 << 27, transcendentals=0),
        name='stage_one',
    )(x_blk, ln_scale, qk_scale, b_up, wq, wu)
    return h


def stage_two_kernel(rows, chips, x_hbm, h_hbm, w_o, w_down, bias, out_hbm, h_v, w_v, x_v, rx_v, half_v, tot_v, ry_v, fin_v,
                     ld_sem, wa_send, wa_recv, wb_send, wb_recv, wc_send, wc_recv, wd_send, wd_recv, hf_send, hf_recv, x_send, x_recv,
                     y_send, y_recv, g_send, g_recv, s_send, s_recv, l_sem):
    p = Place(rows, chips)
    batch, patches, dim_local = x_hbm.shape
    sub = batch // (2 * CORES * chips)
    group = sub * patches
    ko = w_o.shape[0]
    kd = w_down.shape[0]
    order = (0, 1, 2, 3)

    def two(slot, send, recv, who):
        return [remote(w_o, w_v.at[slot, pl.ds(0, ko), :], send.at[0], recv.at[0], who), remote(w_down, w_v.at[slot, pl.ds(ko, kd), :], send.at[1], recv.at[1], who)]

    wa = two(1, wa_send, wa_recv, p.inner_peer)
    wb = two(2, wb_send, wb_recv, p.cross_peer)
    wc = remote(w_v.at[2], w_v.at[3], wc_send, wc_recv, p.inner_peer)
    wd0 = two(0, wd_send, wd_recv, p.sibling)
    wd = [None] + [remote(w_v.at[r], w_v.at[r], wd_send.at[r + 1], wd_recv.at[r + 1], p.sibling) for r in (1, 2, 3)]
    own = [pltpu.make_async_copy(w_o, w_v.at[0, pl.ds(0, ko), :], ld_sem.at[0]), pltpu.make_async_copy(w_down, w_v.at[0, pl.ds(ko, kd), :], ld_sem.at[1])]
    h_copy = pltpu.make_async_copy(h_hbm, h_v, ld_sem.at[2])

    def images(side, dx, core=None):
        half = p.half if side == 0 else 1 - p.half
        return p.first_image(half, dx, p.core if core is None else core, batch)

    fin_load = [pltpu.make_async_copy(x_hbm.at[pl.ds(images(side, 0), sub)], fin_v.at[side], ld_sem.at[3 + side]) for side in (0, 1)]

    def half_copy(q, k):
        who = p.right_peer if k == 0 else p.left_peer
        return remote(x_v.at[q % 2, 3, k], half_v.at[q % 2, k], hf_send.at[q, k], hf_recv.at[q, k], who)

    def x_copy(q, k):
        who = p.right_peer if k == 0 else p.left_peer
        return remote(x_v.at[q % 2, 2 - k], rx_v.at[q % 2, k], x_send.at[q, k], x_recv.at[q, k], who)

    def y_copy(n):
        src, who = ((2, p.cross_peer), (3, p.cross_peer), (1, p.inner_peer))[n]
        return remote(tot_v.at[src], ry_v.at[n], y_send.at[n], y_recv.at[n], who)

    def g_copy(side, k):
        who = p.right_peer if k % 2 == 0 else p.left_peer
        if k < 2:
            src, dst = fin_v.at[side], out_hbm.at[pl.ds(images(side, 0), sub)]
        else:
            image = images(side, chips - 1 if k == 2 else 1) + (k - 2)
            src = dst = out_hbm.at[image]
        return remote(src, dst, g_send.at[side, k], g_recv.at[side, k], who)

    def s_copy(side, k):
        here = out_hbm.at[pl.ds(images(side, (0, chips - 1, 1, 2)[k]), sub)]
        return remote(fin_v.at[side] if k == 0 else here, here, s_send.at[side, k], s_recv.at[side, k], p.sibling)

    def l_copy(side):
        return pltpu.make_async_copy(fin_v.at[side], out_hbm.at[pl.ds(images(side, 0), sub)], l_sem.at[side])

    def compute(q, r):
        s = q % 2
        if q >= 2:
            for k in range(2):
                half_copy(q - 2, k).wait_send()
                x_copy(q - 2, k).wait_send()

        def cell(n, carry):
            rank = lax.rem(n + 3, chips)
            part = jnp.dot(h_v[aligned(rank, group), :], w_v[r], preferred_element_type=jnp.float32).astype(jnp.bfloat16)
            x_v[s, rank] = part.reshape(sub, patches, dim_local)

            @pl.when(n == 0)
            def _():
                half_copy(q, 0).start()
                half_copy(q, 1).start()

            return carry

        lax.fori_loop(0, chips, cell, 0)

    def add(a, b):
        return a.astype(jnp.float32) + b.astype(jnp.float32)

    def mid(q):
        s = q % 2
        half_copy(q, 0).wait_recv()
        half_copy(q, 1).wait_recv()
        for k in range(2):
            x_v[s, 2 - k, k] = add(x_v[s, 2 - k, k], half_v[s, k]).astype(jnp.bfloat16)
            x_copy(q, k).start()

    def reduce(q, r):
        s = q % 2
        x_copy(q, 0).wait_recv()
        x_copy(q, 1).wait_recv()
        for n in range(sub):
            tot_v[r, n] = (add(x_v[s, 0, n], rx_v[s, 0, n]) + rx_v[s, 1, n].astype(jnp.float32)).astype(jnp.bfloat16)
        if r >= 2:
            y_copy(r - 2).start()

    def pass_on():
        y_copy(1).wait_recv()
        for n in range(sub):
            tot_v[1, n] = add(tot_v[1, n], ry_v[1, n]).astype(jnp.bfloat16)
        y_copy(2).start()

    def home(side):
        y_copy(2 if side else 0).wait_recv()
        fin_load[side].wait()
        for n in range(sub):
            total = ry_v[2, n].astype(jnp.float32) if side else add(tot_v[0, n], ry_v[0, n])
            fin_v[side, n] = (fin_v[side, n].astype(jnp.float32) + total + bias[...]).astype(jnp.bfloat16)
        g_copy(side, 0).start()
        g_copy(side, 1).start()
        s_copy(side, 0).start()
        l_copy(side).start()

    def near(side):
        for k in range(2):
            g_copy(side, k).wait_recv()
            g_copy(side, 2 + k).start()
            s_copy(side, 1 + k).start()

    def far(side):
        g_copy(side, 2).wait_recv()
        g_copy(side, 3).wait_recv()
        s_copy(side, 3).start()

    p.enter()

    @pl.when(p.primary)
    def _():
        for c in wa + own + wd0:
            c.start()

    @pl.when(jnp.logical_not(p.primary))
    def _():
        for c in wb:
            c.start()

    h_copy.start()
    for c in fin_load:
        c.start()
    h_copy.wait()

    @pl.when(p.primary)
    def _():
        for c in own:
            c.wait()

    @pl.when(jnp.logical_not(p.primary))
    def _():
        for c in wd0:
            c.wait_recv()

    compute(0, 0)
    mid(0)
    reduce(0, 0)

    @pl.when(p.primary)
    def _():
        for c in wb:
            c.wait_recv()
        wc.start()
        wd[2].start()
        for c in wa:
            c.wait_recv()
        wd[1].start()

    @pl.when(jnp.logical_not(p.primary))
    def _():
        wd[1].wait_recv()

    compute(1, 1)
    mid(1)

    @pl.when(jnp.logical_not(p.primary))
    def _():
        wd[2].wait_recv()

    compute(2, 2)
    mid(2)
    reduce(1, 1)
    reduce(2, 2)

    @pl.when(p.primary)
    def _():
        wc.wait_recv()
        wd[3].start()

    @pl.when(jnp.logical_not(p.primary))
    def _():
        wd[3].wait_recv()

    compute(3, 3)
    mid(3)
    home(0)
    reduce(3, 3)
    near(0)
    pass_on()
    far(0)
    home(1)
    near(1)
    far(1)

    for side in (0, 1):
        for k in range(4):
            s_copy(side, k).wait_recv()
            s_copy(side, k).wait_send()
            g_copy(side, k).wait_send()
        l_copy(side).wait()
    for n in range(3):
        y_copy(n).wait_send()
    for q in (2, 3):
        for k in range(2):
            half_copy(q, k).wait_send()
            x_copy(q, k).wait_send()

    @pl.when(p.primary)
    def _():
        for c in wa + wd0 + [wc] + wd[1:]:
            c.wait_send()

    @pl.when(jnp.logical_not(p.primary))
    def _():
        for c in wb:
            c.wait_send()


def stage_two(rows, chips, x_blk, h, w_o, w_down, b_out):
    batch, patches, dim_local = x_blk.shape
    sub = batch // (2 * CORES * chips)
    k_dim = w_o.shape[0] + w_down.shape[0]
    bf, vm, dma = jnp.bfloat16, pltpu.VMEM, pltpu.SemaphoreType.DMA
    piece = (sub, patches, dim_local)
    anyspec, vmspec = pl.BlockSpec(memory_space=pl.ANY), pl.BlockSpec(memory_space=pltpu.VMEM)
    return pl.pallas_call(
        functools.partial(stage_two_kernel, rows, chips),
        out_shape=jax.ShapeDtypeStruct(x_blk.shape, bf),
        in_specs=[anyspec] * 4 + [vmspec],
        out_specs=anyspec,
        scratch_shapes=[
            vm(h.shape, bf), vm((rows, k_dim, dim_local), bf), vm((2, chips) + piece, bf), vm((2, 2) + piece, bf), vm((2, 2, patches, dim_local), bf),
            vm((rows,) + piece, bf), vm((3,) + piece, bf), vm((2,) + piece, bf),
            dma((5,)), dma((2,)), dma((2,)), dma((2,)), dma((2,)), dma, dma, dma((5,)), dma((5,)), dma((rows, 2)), dma((rows, 2)), dma((rows, 2)), dma((rows, 2)),
            dma((3,)), dma((3,)), dma((2, 4)), dma((2, 4)), dma((2, 4)), dma((2, 4)), dma((2,)),
        ],
        compiler_params=pltpu.CompilerParams(collective_id=1, has_side_effects=True, vmem_limit_bytes=VMEM_MAX),
        cost_estimate=pl.CostEstimate(flops=2 * h.shape[0] * k_dim * dim_local * rows, bytes_accessed=1 << 27, transcendentals=0),
        name='stage_two',
    )(x_blk, h, w_o, w_down, b_out.reshape(1, dim_local))


def solution(mesh):
    rows, cols = mesh.shape['m1'], mesh.shape['m2']
    chips = cols // CORES
    assert rows == 4 and chips == 4

    def local_layer(x_blk, ln_scale, qn_scale, kn_scale, w_qkv, w_up, b_up, w_o, w_down, b_out):
        dim_local = x_blk.shape[2]
        row = lax.axis_index('m1')
        inner, cross = row + 1 - 2 * lax.rem(row, 2), rows - 1 - row
        seen = (row, inner, cross, lax.rem(row + 2, rows))
        scale = jnp.concatenate([lax.dynamic_slice_in_dim(ln_scale, r * dim_local, dim_local) for r in seen])
        h = stage_one(rows, chips, x_blk, scale[None], jnp.stack([qn_scale, kn_scale]), b_up[None], w_qkv.transpose(1, 0, 2), w_up)
        return stage_two(rows, chips, x_blk, h, w_o, w_down, b_out)

    return jax.shard_map(local_layer, mesh=mesh, in_specs=(P('dp', None, 'm1'), P(), P(), P(), P('m1', None, 'm2'), P('m1', 'm2'), P('m2'), P('m2', 'm1'), P('m2', 'm1'), P('m1')), out_specs=P('dp', None, 'm1'), check_vma=False)
```

```python
import functools

import jax
import jax.numpy as jnp
from jax import lax
from jax.experimental import pallas as pl
from jax.experimental.pallas import tpu as pltpu
from jax.sharding import PartitionSpec as P

LN_EPS = 1e-6
CORES = 2
LINES = 16
LANES = 128
AHEAD = 3
CHUNKS = 2
VMEM_MAX = 67043328
MESH = pl.DeviceIdType.MESH


def layer_norm(values, scale):
    mean = jnp.mean(values, axis=-1, keepdims=True)
    centered = values - mean
    variance = jnp.mean(centered * centered, axis=-1, keepdims=True)
    return centered * lax.rsqrt(variance + LN_EPS) * scale


class Place:
    def __init__(self, rows, chips):
        self.rows, self.chips = rows, chips
        self.dp, self.row = lax.axis_index('dp'), lax.axis_index('m1')
        col = lax.axis_index('m2')
        self.col, self.chip, self.core = col, col // CORES, lax.rem(col, CORES)
        self.inner = self.row + 1 - 2 * lax.rem(self.row, 2)
        self.cross = rows - 1 - self.row
        self.pair = self.row // 2
        self.half = lax.rem((self.row + 1) // 2, 2)
        self.primary = self.core == self.pair
        self.inner_peer = (self.dp, self.inner, col)
        self.cross_peer = (self.dp, self.cross, col)
        self.right_peer = (self.dp, self.row, self.at(1) * CORES + self.core)
        self.left_peer = (self.dp, self.row, self.at(chips - 1) * CORES + self.core)
        self.sibling = (self.dp, self.row, self.chip * CORES + 1 - self.core)

    def at(self, dx):
        return lax.rem(self.chip + dx, self.chips)

    def enter(self):
        barrier = pltpu.get_barrier_semaphore()
        partners = (self.inner_peer, self.cross_peer, self.right_peer, self.left_peer, self.sibling)
        for who in partners:
            pl.semaphore_signal(barrier, inc=1, device_id=who, device_id_type=MESH)
        pl.semaphore_wait(barrier, len(partners))

    def first_image(self, half, dx, core, batch):
        per = batch // (2 * CORES)
        return (half * CORES + core) * per + self.at(dx) * (per // self.chips)


def remote(src, dst, ssem, rsem, who):
    return pltpu.make_async_remote_copy(src_ref=src, dst_ref=dst, send_sem=ssem, recv_sem=rsem, device_id=who, device_id_type=MESH)


def aligned(index, size):
    return pl.ds(pl.multiple_of(index * size, size), size)


def stage_one_kernel(rows, chips, heads, x_hbm, ln_scale, qk_scale, bias_own, wq, wu, w_o, w_down, h_hbm, raw, w2_own, w2_cross, u_v, w_v, qkv_v, st_v, up_v, at_v, bias_v,
                     xs_send, xs_recv, ag_send, ag_recv, ld_sem, own_sem, b_send, b_recv, wa_send, wa_recv, wb_send, wb_recv, wc_send, wc_recv,
                     wd_send, wd_recv, up_sem, at_sem, v_send, v_recv):
    p = Place(rows, chips)
    batch, patches, dim_local = x_hbm.shape
    dim = dim_local * rows
    wide = wq.shape[2]
    head_dim = wide // heads
    n_q, n_up = wq.shape[0], wu.shape[1] // wide
    n_w = n_q + n_up
    sub = batch // (2 * CORES * chips)
    group = sub * patches
    dx_of = (0, chips - 1, 1, 2)

    xa = remote(x_hbm.at[pl.ds(p.first_image(p.half, 0, p.core, batch), sub)], raw.at[0, 1], xs_send.at[0], xs_recv.at[0], p.cross_peer)
    xb = remote(x_hbm.at[pl.ds(p.first_image(1 - p.half, 0, p.core, batch), sub)], raw.at[0, 0], xs_send.at[1], xs_recv.at[1], p.inner_peer)
    xc = remote(raw.at[0, 0], raw.at[0, 2], xs_send.at[2], xs_recv.at[2], p.cross_peer)

    def ag(e, k):
        src, dst = ((raw.at[0, e], raw.at[1, e]), (raw.at[0, e], raw.at[2, e]), (raw.at[1, e, 0], raw.at[3, e, 0]), (raw.at[2, e, 1], raw.at[3, e, 1]))[k]
        return remote(src, dst, ag_send.at[e, k], ag_recv.at[e, k], p.right_peer if k % 2 == 0 else p.left_peer)

    def block(r, k):
        return w_v.at[pl.ds(r * dim_local, dim_local), aligned(k, wide)]

    def from_own(k, make, act):
        @pl.when(k < n_q)
        def _():
            act(make(wq.at[jnp.minimum(k, n_q - 1)]))

        @pl.when(k >= n_q)
        def _():
            act(make(wu.at[:, aligned(jnp.maximum(k - n_q, 0), wide)]))

    def wa(k, src=None):
        return remote(block(1, k) if src is None else src, block(1, k), wa_send.at[k], wa_recv.at[k], p.inner_peer)

    def wb(k, src=None):
        return remote(block(2, k) if src is None else src, block(2, k), wb_send.at[k], wb_recv.at[k], p.cross_peer)

    def wc(k):
        return remote(block(2, k), block(3, k), wc_send.at[k], wc_recv.at[k], p.inner_peer)

    def wd(r, k, src=None):
        return remote(block(r, k) if src is None else src, block(r, k), wd_send.at[r, k], wd_recv.at[r, k], p.sibling)

    own_copies = [pltpu.make_async_copy(wq.at[k], block(0, k), own_sem.at[k]) for k in range(n_q)]
    own_copies.append(pltpu.make_async_copy(wu, w_v.at[pl.ds(0, dim_local), pl.ds(n_q * wide, n_up * wide)], own_sem.at[n_q]))
    bias_copy = remote(bias_own, bias_v, b_send, b_recv, p.sibling)

    ko, kd = w_o.shape[0], w_down.shape[0]

    def two(dst, n, who):
        return [remote(w_o, dst.at[pl.ds(0, ko), :], v_send.at[n], v_recv.at[n], who), remote(w_down, dst.at[pl.ds(ko, kd), :], v_send.at[n + 1], v_recv.at[n + 1], who)]

    v_own, v_cross = two(w2_own, 0, p.sibling), two(w2_cross, 2, p.cross_peer)
    v_pass = remote(w2_cross, w2_cross, v_send.at[4], v_recv.at[4], p.sibling)

    def start(copy):
        copy.start()

    def pump(k):
        @pl.when(p.primary)
        def _():
            wb(k).wait_recv()
            wc(k).start()
            wd(2, k).start()
            wa(k).wait_recv()
            wd(1, k).start()
            if k + AHEAD < n_w:
                from_own(k + AHEAD, functools.partial(wa, k + AHEAD), start)
                from_own(k + AHEAD, functools.partial(wd, 0, k + AHEAD), start)

    def hand_over(k):
        @pl.when(p.primary)
        def _():
            wc(k).wait_recv()
            wd(3, k).start()

    def receive(k):
        @pl.when(jnp.logical_not(p.primary))
        def _():
            for r in range(rows):
                wd(r, k).wait_recv()

    def load_copies(rank_dx, rank, s, b):
        image = p.first_image(p.half, rank_dx, p.core, batch) + s
        yield pltpu.make_async_copy(x_hbm.at[image], st_v.at[b, :, pl.ds(0, dim_local)], ld_sem.at[b, 0])
        for e in range(rows - 1):
            yield pltpu.make_async_copy(raw.at[rank, e, s], st_v.at[b, :, pl.ds((e + 1) * dim_local, dim_local)], ld_sem.at[b, e + 1])

    def normalize(ranks):
        jobs = [(rank, s) for rank in ranks for s in range(sub)]
        loads = [list(load_copies(dx_of[rank], rank, s, n % 2)) for n, (rank, s) in enumerate(jobs)]
        for n in range(len(jobs)):
            if n == 0:
                for c in loads[0]:
                    c.start()
            if n + 1 < len(jobs):
                for c in loads[n + 1]:
                    c.start()
            for c in loads[n]:
                c.wait()
            rank, s = jobs[n]

            def lines(m, carry, b=n % 2, base=(rank * sub + s) * patches):
                here = aligned(m, LINES)
                to = pl.ds(pl.multiple_of(base + m * LINES, LINES), LINES)
                parts = [slice(j * LANES, (j + 1) * LANES) for j in range(dim // LANES)]

                def load(part):
                    return st_v[b, here, part].astype(jnp.float32)

                mean = jnp.sum(functools.reduce(jnp.add, [load(part) for part in parts]), axis=-1, keepdims=True) / dim
                squares = [(load(part) - mean) * (load(part) - mean) for part in parts]
                inverse = lax.rsqrt(jnp.sum(functools.reduce(jnp.add, squares), axis=-1, keepdims=True) / dim + LN_EPS)
                for part in parts:
                    u_v[to, part] = ((load(part) - mean) * inverse * ln_scale[:, part]).astype(jnp.bfloat16)
                return carry

            lax.fori_loop(0, patches // LINES, lines, 0, unroll=4)

    def dot_cell(rank, k):
        return jnp.dot(u_v[aligned(rank, group), :], w_v[:, aligned(k, wide)], preferred_element_type=jnp.float32).astype(jnp.bfloat16)

    def qkv_cell(rank, k):
        z = dot_cell(rank, k)
        to = aligned(rank, group)

        @pl.when(k == n_q - 1)
        def _():
            qkv_v[k, to, :] = z

        @pl.when(k < n_q - 1)
        def _():
            scale = qk_scale[pl.ds(k, 1), :]
            for hd in range(heads):
                part = slice(hd * head_dim, (hd + 1) * head_dim)
                qkv_v[k, to, part] = layer_norm(z[:, part].astype(jnp.float32), scale).astype(jnp.bfloat16)

    def at_copy(image, b):
        return pltpu.make_async_copy(at_v.at[b], h_hbm.at[aligned(image, patches), pl.ds(0, wide)], at_sem.at[b])

    def attend(first, count):
        def one(image, carry):
            b = lax.rem(image, 2)
            here = aligned(image, patches)

            @pl.when(image >= 2)
            def _():
                at_copy(image - 2, b).wait()

            for hd in range(heads):
                part = slice(hd * head_dim, (hd + 1) * head_dim)
                q, k, v = (qkv_v[n, here, part] for n in range(3))
                scores = lax.dot_general(q, k, (((1,), (1,)), ((), ())), preferred_element_type=jnp.float32) * head_dim ** -0.5
                probs = jnp.exp(scores - jnp.max(scores, axis=-1, keepdims=True))
                probs = (probs / jnp.sum(probs, axis=-1, keepdims=True)).astype(jnp.bfloat16)
                at_v[b, :, part] = jnp.dot(probs, v, preferred_element_type=jnp.float32).astype(jnp.bfloat16)
            at_copy(image, b).start()
            return carry

        lax.fori_loop(first, first + count, one, 0)

    def up_copy(rank, k, b):
        return pltpu.make_async_copy(up_v.at[b], h_hbm.at[aligned(rank, group), aligned(k - n_q + 1, wide)], up_sem.at[b])

    def up_chunk(k, carry):
        hand_over(k)
        receive(k)

        @pl.when(jnp.logical_and(p.primary, k == n_w - 1))
        def _():
            for c in v_cross:
                c.wait_recv()
            v_pass.start()

        here = aligned(k - n_q, wide)
        bias = jnp.where(p.primary, bias_own[:, here], bias_v[:, here])

        def cell(rank, carry):
            b = lax.rem(rank, 2)

            @pl.when(jnp.logical_or(k > n_q, rank >= 2))
            def _():
                up_copy(rank, k, b).wait()

            m = dot_cell(rank, k).astype(jnp.float32) + bias
            up_v[b] = (0.5 * m * (1.0 + lax.erf(m * 0.5 ** 0.5))).astype(jnp.bfloat16)
            up_copy(rank, k, b).start()
            return carry

        return lax.fori_loop(0, rows, cell, carry)

    p.enter()
    xb.start()
    xa.start()
    bias_copy.start()

    @pl.when(p.primary)
    def _():
        for c in own_copies:
            c.start()
        for k in range(AHEAD):
            from_own(k, functools.partial(wa, k), start)
            from_own(k, functools.partial(wd, 0, k), start)

    @pl.when(jnp.logical_not(p.primary))
    def _():
        from_own(0, functools.partial(wb, 0), start)

    xb.wait_recv()
    xc.start()
    ag(0, 0).start()
    ag(0, 1).start()

    @pl.when(jnp.logical_not(p.primary))
    def _():
        for k in range(1, n_w):
            from_own(k, functools.partial(wb, k), start)
        for c in v_cross:
            c.start()

    xa.wait_recv()
    ag(1, 0).start()
    ag(1, 1).start()
    pump(0)
    xc.wait_recv()
    ag(2, 0).start()
    ag(2, 1).start()
    normalize((0,))

    def forward(e):
        for k in range(2):
            ag(e, k).wait_recv()
            ag(e, 2 + k).start()

    @pl.when(p.primary)
    def _():
        for c in own_copies:
            c.wait()
        for c in v_own:
            c.start()

    def cells(count, job):
        def cell(n, carry):
            qkv_cell(*job(n))
            return carry

        lax.fori_loop(0, count, cell, 0)

    forward(0)
    hand_over(0)
    pump(1)
    forward(1)
    receive(0)
    cells(1, lambda n: (n, n))
    hand_over(1)
    pump(2)
    receive(1)
    cells(1, lambda n: (n, n + 1))
    forward(2)
    normalize((1, 2))
    hand_over(2)
    pump(3)
    receive(2)
    early = (n_q - 1) * 2
    cells(early + rows - 1, lambda n: (jnp.where(n < early, 1 + lax.rem(n, 2), n - early), jnp.where(n < early, n // 2, n_q - 1)))
    pump(4)
    attend(0, (rows - 1) * sub)
    pump(5)
    for e in range(rows - 1):
        ag(e, 2).wait_recv()
        ag(e, 3).wait_recv()
    normalize((rows - 1,))
    cells(n_q, lambda n: (rows - 1, n))
    pump(6)
    attend((rows - 1) * sub, sub)
    bias_copy.wait_recv()
    lax.fori_loop(n_q, n_w, up_chunk, 0)

    for b in range(2):
        at_copy(b, b).wait()
        up_copy(b, n_q, b).wait()
    for c in (xa, xb, xc, bias_copy):
        c.wait_send()
    for e in range(rows - 1):
        for k in range(4):
            ag(e, k).wait_send()

    @pl.when(p.primary)
    def _():
        for k in range(n_w):
            wa(k).wait_send()
            wc(k).wait_send()
            for r in range(rows):
                wd(r, k).wait_send()
        for c in v_own + [v_pass]:
            c.wait_send()

    @pl.when(jnp.logical_not(p.primary))
    def _():
        for k in range(n_w):
            wb(k).wait_send()
        for c in v_cross:
            c.wait_send()
        for c in v_own + [v_pass]:
            c.wait_recv()


def stage_one(rows, chips, x_blk, ln_scale, qk_scale, b_up, wq, wu, w_o, w_down):
    batch, patches, dim_local = x_blk.shape
    dim, wide = rows * dim_local, wq.shape[2]
    heads = wide // qk_scale.shape[1]
    n_q, n_up = wq.shape[0], wu.shape[1] // wide
    n_w = n_q + n_up
    sub = batch // (2 * CORES * chips)
    tokens = chips * sub * patches
    bf, vm, dma = jnp.bfloat16, pltpu.VMEM, pltpu.SemaphoreType.DMA
    anyspec, vmspec = pl.BlockSpec(memory_space=pl.ANY), pl.BlockSpec(memory_space=pltpu.VMEM)
    w2 = jax.ShapeDtypeStruct((w_o.shape[0] + w_down.shape[0], dim_local), bf)
    h, _, w2_own, w2_cross = pl.pallas_call(
        functools.partial(stage_one_kernel, rows, chips, heads),
        out_shape=(jax.ShapeDtypeStruct((tokens, wide + n_up * wide), bf), jax.ShapeDtypeStruct((chips, rows - 1, sub, patches, dim_local), bf), w2, w2),
        in_specs=[anyspec, vmspec, vmspec, vmspec] + [anyspec] * 4,
        out_specs=(anyspec,) * 4,
        scratch_shapes=[
            vm((tokens, dim), bf), vm((dim, n_w * wide), bf), vm((n_q, tokens, wide), bf), vm((2, patches, dim), bf),
            vm((2, sub * patches, wide), bf), vm((2, patches, wide), bf), vm(b_up.shape, jnp.float32),
            dma((3,)), dma((3,)), dma((rows - 1, 4)), dma((rows - 1, 4)), dma((2, rows)), dma((n_q + 1,)), dma, dma,
            dma((n_w,)), dma((n_w,)), dma((n_w,)), dma((n_w,)), dma((n_w,)), dma((n_w,)), dma((rows, n_w)), dma((rows, n_w)), dma((2,)), dma((2,)), dma((5,)), dma((5,)),
        ],
        compiler_params=pltpu.CompilerParams(collective_id=0, has_side_effects=True, vmem_limit_bytes=VMEM_MAX),
        cost_estimate=pl.CostEstimate(flops=2 * tokens * dim * n_w * wide, bytes_accessed=1 << 27, transcendentals=0),
        name='stage_one',
    )(x_blk, ln_scale, qk_scale, b_up, wq, wu, w_o, w_down)
    return h, w2_own, w2_cross


def stage_two_kernel(rows, chips, x_hbm, h_hbm, w_o, w_down, w2_own, w2_cross, bias, out_hbm, h_v, w_v, ys_v, yt_v, x_v, rx_v, half_v, tot_v, t2_v, in_v, fin_v,
                     ld_sem, wa_send, wa_recv, wc_send, wc_recv, wd_send, wd_recv, hf_send, hf_recv, x_send, x_recv, p_send, p_recv, t_send, t_recv,
                     i_send, i_recv, g_send, g_recv, s_send, s_recv, l_sem):
    p = Place(rows, chips)
    batch, patches, dim_local = x_hbm.shape
    sub = batch // (2 * CORES * chips)
    group = sub * patches
    ko, kd = w_o.shape[0], w_down.shape[0]
    cw = dim_local // CHUNKS
    far_rank = rows - 1

    def cols(c):
        return pl.ds(c * cw, cw)

    def two(c, slot, make):
        return [make(w_o.at[:, cols(c)], w_v.at[c, slot, pl.ds(0, ko), :], 0), make(w_down.at[:, cols(c)], w_v.at[c, slot, pl.ds(ko, kd), :], 1)]

    wa = [two(c, 1, lambda s, d, n, c=c: remote(s, d, wa_send.at[c, n], wa_recv.at[c, n], p.inner_peer)) for c in range(CHUNKS)]
    wc = [remote(w2_cross.at[:, cols(c)], w_v.at[c, 3], wc_send.at[c], wc_recv.at[c], p.inner_peer) for c in range(CHUNKS)]
    wd = [{r: remote(w_v.at[c, r], w_v.at[c, r], wd_send.at[c, r // 2], wd_recv.at[c, r // 2], p.sibling) for r in (1, 3)} for c in range(CHUNKS)]
    own_primary = [two(c, 0, lambda s, d, n, c=c: pltpu.make_async_copy(s, d, ld_sem.at[2 * c + n])) for c in range(CHUNKS)]
    own_other = [pltpu.make_async_copy(w2_own.at[:, cols(c)], w_v.at[c, 0], ld_sem.at[2 * c]) for c in range(CHUNKS)]
    cross_load = [pltpu.make_async_copy(w2_cross.at[:, cols(c)], w_v.at[c, 2], ld_sem.at[2 * CHUNKS + c]) for c in range(CHUNKS)]
    h_copy = pltpu.make_async_copy(h_hbm, h_v, ld_sem.at[3 * CHUNKS])

    def images(side, dx):
        return p.first_image(p.half if side == 0 else 1 - p.half, dx, p.core, batch)

    fin_load = [
        [pltpu.make_async_copy(x_hbm.at[pl.ds(images(side, 0), sub), :, cols(c)], fin_v.at[side, c], ld_sem.at[3 * CHUNKS + 1 + side * CHUNKS + c]) for c in range(CHUNKS)]
        for side in (0, 1)
    ]

    def p_copy(c, rank):
        return remote(ys_v.at[c, rank], yt_v.at[c, rank], p_send.at[c, rank], p_recv.at[c, rank], p.cross_peer)

    def half_copy(u, k):
        who = p.right_peer if k == 0 else p.left_peer
        return remote(x_v.at[u % 3, far_rank, k], half_v.at[u, k], hf_send.at[u, k], hf_recv.at[u, k], who)

    def x_copy(u, k):
        who = p.right_peer if k == 0 else p.left_peer
        return remote(x_v.at[u % 3, 2 - k], rx_v.at[u, k], x_send.at[u, k], x_recv.at[u, k], who)

    def t_copy(c):
        return remote(tot_v.at[1, c], t2_v.at[c], t_send.at[c], t_recv.at[c], p.cross_peer)

    def i_copy(c):
        return remote(tot_v.at[2, c], in_v.at[c], i_send.at[c], i_recv.at[c], p.inner_peer)

    def spot(side, dx, c, count=sub, first=0):
        return out_hbm.at[pl.ds(images(side, dx) + first, count), :, cols(c)]

    def g_copy(side, c, k):
        who = p.right_peer if k % 2 == 0 else p.left_peer
        if k < 2:
            src, dst = fin_v.at[side, c], spot(side, 0, c)
        else:
            src = dst = spot(side, chips - 1 if k == 2 else 1, c, 1, k - 2)
        return remote(src, dst, g_send.at[side, c, k], g_recv.at[side, c, k], who)

    def s_copy(side, c, k):
        here = spot(side, (0, chips - 1, 1, 2)[k], c)
        return remote(fin_v.at[side, c] if k == 0 else here, here, s_send.at[side, c, k], s_recv.at[side, c, k], p.sibling)

    def l_copy(side, c):
        return pltpu.make_async_copy(fin_v.at[side, c], spot(side, 0, c), l_sem.at[side, c])

    def add(a, b):
        return a.astype(jnp.float32) + b.astype(jnp.float32)

    def dot(rank, c, r):
        return jnp.dot(h_v[aligned(rank, group), :], w_v[c, r], preferred_element_type=jnp.float32).astype(jnp.bfloat16).reshape(sub, patches, cw)

    def received(c, r):
        if r in (1, 3):

            @pl.when(jnp.logical_not(p.primary))
            def _():
                wd[c][r].wait_recv()

    def cross_part(c, r):
        received(c, r)

        def cell(n, carry):
            rank = far_rank - n
            ys_v[c, rank] = dot(rank, c, r)
            p_copy(c, rank).start()
            return carry

        lax.fori_loop(0, chips, cell, 0)

    def reuse(u):
        if u >= 3:
            for k in range(2):
                half_copy(u - 3, k).wait_send()
                x_copy(u - 3, k).wait_send()

    def mid_one(u, k):
        half_copy(u, k).wait_recv()
        s = u % 3
        x_v[s, 2 - k, k] = add(x_v[s, 2 - k, k], half_v[u, k]).astype(jnp.bfloat16)
        x_copy(u, k).start()

    def pair_part(u, c, r):
        reuse(u)
        s = u % 3
        received(c, r)

        def cell(n, carry):
            rank = far_rank - n
            part = dot(rank, c, r)
            p_copy(c, rank).wait_recv()
            x_v[s, rank] = add(part, yt_v[c, rank]).astype(jnp.bfloat16)

            @pl.when(n == 0)
            def _():
                half_copy(u, 0).start()
                half_copy(u, 1).start()

            for k in range(2):

                @pl.when(n == k + 1)
                def _(k=k):
                    mid_one(u, k)

            return carry

        lax.fori_loop(0, chips, cell, 0)

    def compute(u, c, r):
        reuse(u)
        s = u % 3
        received(c, r)

        def cell(n, carry):
            rank = far_rank - n
            x_v[s, rank] = dot(rank, c, r)

            @pl.when(n == 0)
            def _():
                half_copy(u, 0).start()
                half_copy(u, 1).start()

            return carry

        lax.fori_loop(0, chips, cell, 0)

    def mid(u):
        mid_one(u, 0)
        mid_one(u, 1)

    def total(u, n):
        s = u % 3
        return add(x_v[s, 0, n], rx_v[u, 0, n]) + rx_v[u, 1, n].astype(jnp.float32)

    def arrived(u):
        x_copy(u, 0).wait_recv()
        x_copy(u, 1).wait_recv()

    def reduce(u, c, slot, send=None):
        arrived(u)
        for n in range(sub):
            tot_v[slot, c, n] = total(u, n).astype(jnp.bfloat16)
        if send is not None:
            send(c).start()

    def fetch_far(c):
        @pl.when(p.primary)
        def _():
            wc[c].wait_recv()
            wd[c][3].start()

    def fetch_inner(c):
        @pl.when(p.primary)
        def _():
            for copy in wa[c]:
                copy.wait_recv()
            wd[c][1].start()

    def pass_on(c):
        t_copy(c).wait_recv()
        for n in range(sub):
            tot_v[2, c, n] = add(tot_v[0, c, n], t2_v[c, n]).astype(jnp.bfloat16)
        i_copy(c).start()

    def home(side, c, u=None):
        if u is None:
            (i_copy if side else t_copy)(c).wait_recv()
        else:
            arrived(u)
        fin_load[side][c].wait()
        for n in range(sub):
            if u is not None:
                summed = total(u, n)
            else:
                summed = in_v[c, n].astype(jnp.float32) if side else add(tot_v[0, c, n], t2_v[c, n])
            fin_v[side, c, n] = (fin_v[side, c, n].astype(jnp.float32) + summed + bias[:, cols(c)]).astype(jnp.bfloat16)
        g_copy(side, c, 0).start()
        g_copy(side, c, 1).start()
        s_copy(side, c, 0).start()
        l_copy(side, c).start()

    def near(side, c):
        for k in range(2):
            g_copy(side, c, k).wait_recv()
            g_copy(side, c, 2 + k).start()
            s_copy(side, c, 1 + k).start()

    def far(side, c):
        g_copy(side, c, 2).wait_recv()
        g_copy(side, c, 3).wait_recv()
        s_copy(side, c, 3).start()

    h_copy.start()
    for c in range(CHUNKS):
        cross_load[c].start()

        @pl.when(p.primary)
        def _(c=c):
            for copy in own_primary[c]:
                copy.start()

        @pl.when(jnp.logical_not(p.primary))
        def _(c=c):
            own_other[c].start()

    for side in (0, 1):
        for c in range(CHUNKS):
            fin_load[side][c].start()
    p.enter()

    @pl.when(p.primary)
    def _():
        for copy in [wc[1], wc[0]] + wa[0] + wa[1]:
            copy.start()

    h_copy.wait()
    for c in range(CHUNKS):

        @pl.when(p.primary)
        def _(c=c):
            for copy in own_primary[c]:
                copy.wait()

        @pl.when(jnp.logical_not(p.primary))
        def _(c=c):
            own_other[c].wait()

        cross_load[c].wait()

    cross_part(0, 2)
    compute(0, 1, 0)
    compute(1, 1, 2)
    mid(0)
    mid(1)
    reduce(0, 1, 0)
    fetch_far(1)
    pair_part(2, 0, 0)
    reduce(1, 1, 1, t_copy)
    cross_part(1, 3)
    fetch_far(0)
    compute(3, 0, 3)
    home(0, 1)
    home(0, 0, 2)
    mid(3)
    near(0, 1)
    near(0, 0)
    reduce(3, 0, 1, t_copy)
    fetch_inner(0)
    compute(4, 0, 1)
    far(0, 1)
    mid(4)
    far(0, 0)
    reduce(4, 0, 0)
    fetch_inner(1)
    pass_on(0)
    pair_part(5, 1, 1)
    home(1, 0)
    reduce(5, 1, 2, i_copy)
    near(1, 0)
    home(1, 1)
    far(1, 0)
    near(1, 1)
    far(1, 1)

    for c in range(CHUNKS):
        for side in (0, 1):
            for k in range(4):
                s_copy(side, c, k).wait_recv()
                s_copy(side, c, k).wait_send()
                g_copy(side, c, k).wait_send()
            l_copy(side, c).wait()
        t_copy(c).wait_send()
        i_copy(c).wait_send()
        for rank in range(chips):
            p_copy(c, rank).wait_send()
    for u in (3, 4, 5):
        for k in range(2):
            half_copy(u, k).wait_send()
            x_copy(u, k).wait_send()

    @pl.when(p.primary)
    def _():
        for c in range(CHUNKS):
            wc[c].wait_send()
            for copy in wa[c]:
                copy.wait_send()
            for r in (1, 3):
                wd[c][r].wait_send()


def stage_two(rows, chips, x_blk, h, w_o, w_down, w2_own, w2_cross, b_out):
    batch, patches, dim_local = x_blk.shape
    sub = batch // (2 * CORES * chips)
    k_dim, cw = w2_own.shape[0], dim_local // CHUNKS
    units = 3 * CHUNKS
    bf, vm, dma = jnp.bfloat16, pltpu.VMEM, pltpu.SemaphoreType.DMA
    piece = (sub, patches, cw)
    anyspec, vmspec = pl.BlockSpec(memory_space=pl.ANY), pl.BlockSpec(memory_space=pltpu.VMEM)
    return pl.pallas_call(
        functools.partial(stage_two_kernel, rows, chips),
        out_shape=jax.ShapeDtypeStruct(x_blk.shape, bf),
        in_specs=[anyspec] * 6 + [vmspec],
        out_specs=anyspec,
        scratch_shapes=[
            vm(h.shape, bf), vm((CHUNKS, rows, k_dim, cw), bf), vm((CHUNKS, chips) + piece, bf), vm((CHUNKS, chips) + piece, bf), vm((3, chips) + piece, bf),
            vm((units, 2) + piece, bf), vm((units, 2, patches, cw), bf), vm((3, CHUNKS) + piece, bf), vm((CHUNKS,) + piece, bf), vm((CHUNKS,) + piece, bf),
            vm((2, CHUNKS) + piece, bf),
            dma((5 * CHUNKS + 1,)), dma((CHUNKS, 2)), dma((CHUNKS, 2)), dma((CHUNKS,)), dma((CHUNKS,)), dma((CHUNKS, 2)), dma((CHUNKS, 2)),
            dma((units, 2)), dma((units, 2)), dma((units, 2)), dma((units, 2)), dma((CHUNKS, chips)), dma((CHUNKS, chips)), dma((CHUNKS,)), dma((CHUNKS,)),
            dma((CHUNKS,)), dma((CHUNKS,)), dma((2, CHUNKS, 4)), dma((2, CHUNKS, 4)), dma((2, CHUNKS, 4)), dma((2, CHUNKS, 4)), dma((2, CHUNKS)),
        ],
        compiler_params=pltpu.CompilerParams(collective_id=1, has_side_effects=True, vmem_limit_bytes=VMEM_MAX),
        cost_estimate=pl.CostEstimate(flops=2 * h.shape[0] * k_dim * dim_local * rows, bytes_accessed=1 << 27, transcendentals=0),
        name='stage_two',
    )(x_blk, h, w_o, w_down, w2_own, w2_cross, b_out.reshape(1, dim_local))


def solution(mesh):
    rows, cols = mesh.shape['m1'], mesh.shape['m2']
    chips = cols // CORES
    assert rows == 4 and chips == 4

    def local_layer(x_blk, ln_scale, qn_scale, kn_scale, w_qkv, w_up, b_up, w_o, w_down, b_out):
        dim_local = x_blk.shape[2]
        row = lax.axis_index('m1')
        inner, cross = row + 1 - 2 * lax.rem(row, 2), rows - 1 - row
        seen = (row, inner, cross, lax.rem(row + 2, rows))
        scale = jnp.concatenate([lax.dynamic_slice_in_dim(ln_scale, r * dim_local, dim_local) for r in seen])
        h, w2_own, w2_cross = stage_one(rows, chips, x_blk, scale[None], jnp.stack([qn_scale, kn_scale]), b_up[None], w_qkv.transpose(1, 0, 2), w_up, w_o, w_down)
        return stage_two(rows, chips, x_blk, h, w_o, w_down, w2_own, w2_cross, b_out)

    return jax.shard_map(local_layer, mesh=mesh, in_specs=(P('dp', None, 'm1'), P(), P(), P(), P('m1', None, 'm2'), P('m1', 'm2'), P('m2'), P('m2', 'm1'), P('m2', 'm1'), P('m1')), out_specs=P('dp', None, 'm1'), check_vma=False)
```

```python
import functools

import jax
import jax.numpy as jnp
from jax import lax
from jax.experimental import pallas as pl
from jax.experimental.pallas import tpu as pltpu
from jax.sharding import PartitionSpec as P

LN_EPS = 1e-6
CORES = 2
LINES = 16
LANES = 128
AHEAD = 2
CHUNKS = 2
VMEM_MAX = 67043328
MESH = pl.DeviceIdType.MESH


def layer_norm(values, scale):
    mean = jnp.mean(values, axis=-1, keepdims=True)
    centered = values - mean
    variance = jnp.mean(centered * centered, axis=-1, keepdims=True)
    return centered * lax.rsqrt(variance + LN_EPS) * scale


class Place:
    def __init__(self, rows, chips):
        self.rows, self.chips = rows, chips
        self.dp, self.row = lax.axis_index('dp'), lax.axis_index('m1')
        col = lax.axis_index('m2')
        self.col, self.chip, self.core = col, col // CORES, lax.rem(col, CORES)
        self.inner = self.row + 1 - 2 * lax.rem(self.row, 2)
        self.cross = rows - 1 - self.row
        self.pair = self.row // 2
        self.half = lax.rem((self.row + 1) // 2, 2)
        self.primary = self.core == self.pair
        self.inner_peer = (self.dp, self.inner, col)
        self.cross_peer = (self.dp, self.cross, col)
        self.right_peer = (self.dp, self.row, self.at(1) * CORES + self.core)
        self.left_peer = (self.dp, self.row, self.at(chips - 1) * CORES + self.core)
        self.sibling = (self.dp, self.row, self.chip * CORES + 1 - self.core)

    def at(self, dx):
        return lax.rem(self.chip + dx, self.chips)

    def enter(self):
        barrier = pltpu.get_barrier_semaphore()
        partners = (self.inner_peer, self.cross_peer, self.right_peer, self.left_peer, self.sibling)
        for who in partners:
            pl.semaphore_signal(barrier, inc=1, device_id=who, device_id_type=MESH)
        pl.semaphore_wait(barrier, len(partners))

    def first_image(self, half, dx, core, batch):
        per = batch // (2 * CORES)
        return (half * CORES + core) * per + self.at(dx) * (per // self.chips)


def remote(src, dst, ssem, rsem, who):
    return pltpu.make_async_remote_copy(src_ref=src, dst_ref=dst, send_sem=ssem, recv_sem=rsem, device_id=who, device_id_type=MESH)


def aligned(index, size):
    return pl.ds(pl.multiple_of(index * size, size), size)


def stage_one_kernel(rows, chips, heads, x_hbm, ln_all, qn_scale, kn_scale, bias_own, wq, wu, w_o, w_down, h_hbm, raw, w2_own, w2_cross, u_v, w_v, qkv_v, st_v, up_v, last_v, at_v, bias_v, ln_scale,
                     xs_send, xs_recv, ag_send, ag_recv, ld_sem, own_sem, b_send, b_recv, wa_send, wa_recv, wb_send, wb_recv, wc_send, wc_recv,
                     wd_send, wd_recv, up_sem, at_sem, v_send, v_recv, last_sem):
    p = Place(rows, chips)
    batch, patches, dim_local = x_hbm.shape
    dim = dim_local * rows
    wide = wq.shape[2]
    head_dim = wide // heads
    n_q, n_up = wq.shape[0], wu.shape[1] // wide
    n_w = n_q + n_up
    sub = batch // (2 * CORES * chips)
    group = sub * patches
    dx_of = (0, chips - 1, 1, 2)

    xa = remote(x_hbm.at[pl.ds(p.first_image(p.half, 0, p.core, batch), sub)], raw.at[0, 1], xs_send.at[0], xs_recv.at[0], p.cross_peer)
    xb = remote(x_hbm.at[pl.ds(p.first_image(1 - p.half, 0, p.core, batch), sub)], raw.at[0, 0], xs_send.at[1], xs_recv.at[1], p.inner_peer)
    xc = remote(raw.at[0, 0], raw.at[0, 2], xs_send.at[2], xs_recv.at[2], p.cross_peer)

    def ag(e, k):
        src, dst = ((raw.at[0, e], raw.at[1, e]), (raw.at[0, e], raw.at[2, e]), (raw.at[1, e, 0], raw.at[3, e, 0]), (raw.at[2, e, 1], raw.at[3, e, 1]))[k]
        return remote(src, dst, ag_send.at[e, k], ag_recv.at[e, k], p.right_peer if k % 2 == 0 else p.left_peer)

    def block(r, k):
        return w_v.at[pl.ds(r * dim_local, dim_local), aligned(k, wide)]

    def from_own(k, make, act):
        @pl.when(k < n_q)
        def _():
            act(make(wq.at[jnp.minimum(k, n_q - 1)]))

        @pl.when(k >= n_q)
        def _():
            act(make(wu.at[:, aligned(jnp.maximum(k - n_q, 0), wide)]))

    def wa(k, src=None):
        return remote(block(1, k) if src is None else src, block(1, k), wa_send.at[k], wa_recv.at[k], p.inner_peer)

    def wb(k, src=None):
        return remote(block(2, k) if src is None else src, block(2, k), wb_send.at[k], wb_recv.at[k], p.cross_peer)

    def wc(k):
        return remote(block(2, k), block(3, k), wc_send.at[k], wc_recv.at[k], p.inner_peer)

    def wd(r, k, src=None):
        return remote(block(r, k) if src is None else src, block(r, k), wd_send.at[r, k], wd_recv.at[r, k], p.sibling)

    own_copies = [pltpu.make_async_copy(wq.at[k], block(0, k), own_sem.at[k]) for k in range(n_q)]
    own_copies.append(pltpu.make_async_copy(wu, w_v.at[pl.ds(0, dim_local), pl.ds(n_q * wide, n_up * wide)], own_sem.at[n_q]))
    bias_copy = remote(bias_own, bias_v, b_send, b_recv, p.sibling)

    ko, kd = w_o.shape[0], w_down.shape[0]

    def two(dst, n, who):
        return [remote(w_o, dst.at[pl.ds(0, ko), :], v_send.at[n], v_recv.at[n], who), remote(w_down, dst.at[pl.ds(ko, kd), :], v_send.at[n + 1], v_recv.at[n + 1], who)]

    v_own, v_cross = two(w2_own, 0, p.sibling), two(w2_cross, 2, p.cross_peer)

    for r, source in enumerate((p.row, p.inner, p.cross, lax.rem(p.row + 2, rows))):
        ln_scale[:, r * dim_local : (r + 1) * dim_local] = ln_all[:, aligned(source, dim_local)]

    def start(copy):
        copy.start()

    def pump(k):
        @pl.when(p.primary)
        def _():
            wb(k).wait_recv()
            for c in wc_last if k == n_w - 1 else [wc(k)]:
                c.start()
            wd(2, k).start()
            if k + AHEAD < n_w:
                from_own(k + AHEAD, functools.partial(wa, k + AHEAD), start)
                from_own(k + AHEAD, functools.partial(wd, 0, k + AHEAD), start)

    def last_half(r, n):
        return w_v.at[pl.ds(r * dim_local, dim_local), pl.ds((n_w - 1) * wide + n * (wide // 2), wide // 2)]

    wc_last = [remote(last_half(2, n), last_half(3, n), wc_send.at[n_w - 1 + n], wc_recv.at[n_w - 1 + n], p.inner_peer) for n in range(2)]
    wd_last = [remote(last_half(3, n), last_half(3, n), wd_send.at[n, n_w], wd_recv.at[n, n_w], p.sibling) for n in range(2)]

    def hand_over(k):
        @pl.when(p.primary)
        def _():
            wa(k).wait_recv()
            wd(1, k).start()
            wc(k).wait_recv()
            wd(3, k).start()

    def receive(k):
        @pl.when(jnp.logical_not(p.primary))
        def _():
            for r in range(rows):
                wd(r, k).wait_recv()

    def load_copies(rank_dx, rank, s, b):
        image = p.first_image(p.half, rank_dx, p.core, batch) + s
        yield pltpu.make_async_copy(x_hbm.at[image], st_v.at[b, :, pl.ds(0, dim_local)], ld_sem.at[b, 0])
        for e in range(rows - 1):
            yield pltpu.make_async_copy(raw.at[rank, e, s], st_v.at[b, :, pl.ds((e + 1) * dim_local, dim_local)], ld_sem.at[b, e + 1])

    def normalize(ranks):
        jobs = [(rank, s) for rank in ranks for s in range(sub)]
        loads = [list(load_copies(dx_of[rank], rank, s, n % 2)) for n, (rank, s) in enumerate(jobs)]
        for n in range(len(jobs)):
            if n == 0:
                for c in loads[0]:
                    c.start()
            if n + 1 < len(jobs):
                for c in loads[n + 1]:
                    c.start()
            for c in loads[n]:
                c.wait()
            rank, s = jobs[n]

            def lines(m, carry, b=n % 2, base=(rank * sub + s) * patches):
                here = aligned(m, LINES)
                to = pl.ds(pl.multiple_of(base + m * LINES, LINES), LINES)
                parts = [slice(j * LANES, (j + 1) * LANES) for j in range(dim // LANES)]

                def load(part):
                    return st_v[b, here, part].astype(jnp.float32)

                mean = jnp.sum(functools.reduce(jnp.add, [load(part) for part in parts]), axis=-1, keepdims=True) / dim
                squares = [(load(part) - mean) * (load(part) - mean) for part in parts]
                inverse = lax.rsqrt(jnp.sum(functools.reduce(jnp.add, squares), axis=-1, keepdims=True) / dim + LN_EPS)
                for part in parts:
                    u_v[to, part] = ((load(part) - mean) * inverse * ln_scale[:, part]).astype(jnp.bfloat16)
                return carry

            lax.fori_loop(0, patches // LINES, lines, 0, unroll=4)

    def dot_cell(rank, k):
        return jnp.dot(u_v[aligned(rank, group), :], w_v[:, aligned(k, wide)], preferred_element_type=jnp.float32).astype(jnp.bfloat16)

    def qkv_cell(rank, k):
        z = dot_cell(rank, k)
        to = aligned(rank, group)

        @pl.when(k == n_q - 1)
        def _():
            qkv_v[k, to, :] = z

        @pl.when(k < n_q - 1)
        def _():
            scale = jnp.where(k == 0, qn_scale[...], kn_scale[...])
            for hd in range(heads):
                part = slice(hd * head_dim, (hd + 1) * head_dim)
                qkv_v[k, to, part] = layer_norm(z[:, part].astype(jnp.float32), scale).astype(jnp.bfloat16)

    def at_copy(image, b):
        return pltpu.make_async_copy(at_v.at[b], h_hbm.at[aligned(image, patches), pl.ds(0, wide)], at_sem.at[b])

    def attend(first, count):
        def one(image, carry):
            b = lax.rem(image, 2)
            here = aligned(image, patches)

            @pl.when(image >= 2)
            def _():
                at_copy(image - 2, b).wait()

            for hd in range(heads):
                part = slice(hd * head_dim, (hd + 1) * head_dim)
                q, k, v = (qkv_v[n, here, part] for n in range(3))
                scores = lax.dot_general(q, k, (((1,), (1,)), ((), ())), preferred_element_type=jnp.float32) * head_dim ** -0.5
                probs = jnp.exp(scores - jnp.max(scores, axis=-1, keepdims=True))
                probs = (probs / jnp.sum(probs, axis=-1, keepdims=True)).astype(jnp.bfloat16)
                at_v[b, :, part] = jnp.dot(probs, v, preferred_element_type=jnp.float32).astype(jnp.bfloat16)
            at_copy(image, b).start()
            return carry

        lax.fori_loop(first, first + count, one, 0)

    def up_copy(rank, k, b):
        return pltpu.make_async_copy(up_v.at[b], h_hbm.at[aligned(rank, group), aligned(k - n_q + 1, wide)], up_sem.at[b])

    def bias_of(here):
        return jnp.where(p.primary, bias_own[:, here], bias_v[:, here])

    def up_chunk(k, carry):
        hand_over(k)
        receive(k)
        bias = bias_of(aligned(k - n_q, wide))

        def cell(rank, carry):
            b = lax.rem(rank, 2)

            @pl.when(jnp.logical_or(k > n_q, rank >= 2))
            def _():
                up_copy(rank, k, b).wait()

            m = dot_cell(rank, k).astype(jnp.float32) + bias
            up_v[b] = (0.5 * m * (1.0 + lax.erf(m * 0.5 ** 0.5))).astype(jnp.bfloat16)
            up_copy(rank, k, b).start()
            return carry

        return lax.fori_loop(0, rows, cell, carry)

    def last_copy(rank, n):
        to = pl.ds(wide + (n_up - 1) * wide + n * (wide // 2), wide // 2)
        return pltpu.make_async_copy(last_v.at[n, lax.rem(rank, 2)], h_hbm.at[aligned(rank, group), to], last_sem.at[n, lax.rem(rank, 2)])

    def last_chunk(n):
        @pl.when(p.primary)
        def _():
            if n == 0:
                wa(n_w - 1).wait_recv()
                wd(1, n_w - 1).start()
            wc_last[n].wait_recv()
            wd_last[n].start()
            if n == 0:
                for c in v_cross:
                    c.wait_recv()

        @pl.when(jnp.logical_not(p.primary))
        def _():
            if n == 0:
                for r in range(rows - 1):
                    wd(r, n_w - 1).wait_recv()
            wd_last[n].wait_recv()

        first = (n_up - 1) * wide + n * (wide // 2)
        bias = bias_of(pl.ds(first, wide // 2))
        weight = pl.ds(n_q * wide + first, wide // 2)

        def cell(rank, carry):
            @pl.when(rank >= 2)
            def _():
                last_copy(rank - 2, n).wait()

            m = jnp.dot(u_v[aligned(rank, group), :], w_v[:, weight], preferred_element_type=jnp.float32).astype(jnp.bfloat16).astype(jnp.float32) + bias
            last_v[n, lax.rem(rank, 2)] = (0.5 * m * (1.0 + lax.erf(m * 0.5 ** 0.5))).astype(jnp.bfloat16)
            last_copy(rank, n).start()
            return carry

        lax.fori_loop(0, rows, cell, 0)

    p.enter()
    xb.start()

    @pl.when(jnp.logical_not(p.primary))
    def _():
        from_own(0, functools.partial(wb, 0), start)

    xa.start()
    bias_copy.start()

    @pl.when(p.primary)
    def _():
        for c in own_copies:
            c.start()
        for k in range(AHEAD):
            from_own(k, functools.partial(wa, k), start)
            from_own(k, functools.partial(wd, 0, k), start)

    xb.wait_recv()
    xc.start()
    ag(0, 0).start()
    ag(0, 1).start()

    @pl.when(jnp.logical_not(p.primary))
    def _():
        for k in range(1, n_w):
            from_own(k, functools.partial(wb, k), start)
        for c in v_cross:
            c.start()

    xa.wait_recv()
    ag(1, 0).start()
    ag(1, 1).start()
    pump(0)
    xc.wait_recv()
    ag(2, 0).start()
    ag(2, 1).start()
    normalize((0,))

    def forward(e):
        for k in range(2):
            ag(e, k).wait_recv()
            ag(e, 2 + k).start()

    @pl.when(p.primary)
    def _():
        for c in own_copies:
            c.wait()
        for c in v_own:
            c.start()

    def cells(count, job):
        def cell(n, carry):
            qkv_cell(*job(n))
            return carry

        lax.fori_loop(0, count, cell, 0)

    forward(0)
    hand_over(0)
    pump(1)
    forward(1)
    receive(0)
    cells(1, lambda n: (n, n))
    hand_over(1)
    pump(2)
    receive(1)
    cells(1, lambda n: (n, n + 1))
    forward(2)
    normalize((1, 2))
    hand_over(2)
    pump(3)
    receive(2)
    early = (n_q - 1) * 2
    cells(early + rows - 1, lambda n: (jnp.where(n < early, 1 + lax.rem(n, 2), n - early), jnp.where(n < early, n // 2, n_q - 1)))
    pump(4)
    attend(0, (rows - 1) * sub)
    pump(5)
    for e in range(rows - 1):
        ag(e, 2).wait_recv()
        ag(e, 3).wait_recv()
    normalize((rows - 1,))
    cells(n_q, lambda n: (rows - 1, n))
    pump(6)
    attend((rows - 1) * sub, sub)
    bias_copy.wait_recv()
    lax.fori_loop(n_q, n_w - 1, up_chunk, 0)
    last_chunk(0)
    last_chunk(1)

    for b in range(2):
        at_copy(b, b).wait()
        up_copy(b, n_q, b).wait()
        for n in range(2):
            last_copy(b, n).wait()
    for c in (xa, xb, xc, bias_copy):
        c.wait_send()
    for e in range(rows - 1):
        for k in range(4):
            ag(e, k).wait_send()

    @pl.when(p.primary)
    def _():
        for k in range(n_w):
            wa(k).wait_send()
            if k < n_w - 1:
                wc(k).wait_send()
            for r in range(rows if k < n_w - 1 else rows - 1):
                wd(r, k).wait_send()
        for c in v_own + wc_last + wd_last:
            c.wait_send()

    @pl.when(jnp.logical_not(p.primary))
    def _():
        for k in range(n_w):
            wb(k).wait_send()
        for c in v_cross:
            c.wait_send()
        for c in v_own:
            c.wait_recv()


def stage_one(rows, chips, x_blk, ln_scale, qn_scale, kn_scale, b_up, wq, wu, w_o, w_down):
    batch, patches, dim_local = x_blk.shape
    dim, wide = rows * dim_local, wq.shape[2]
    heads = wide // qn_scale.shape[1]
    n_q, n_up = wq.shape[0], wu.shape[1] // wide
    n_w = n_q + n_up
    sub = batch // (2 * CORES * chips)
    tokens = chips * sub * patches
    bf, vm, dma = jnp.bfloat16, pltpu.VMEM, pltpu.SemaphoreType.DMA
    anyspec, vmspec = pl.BlockSpec(memory_space=pl.ANY), pl.BlockSpec(memory_space=pltpu.VMEM)
    w2 = jax.ShapeDtypeStruct((w_o.shape[0] + w_down.shape[0], dim_local), bf)
    h, _, w2_own, w2_cross = pl.pallas_call(
        functools.partial(stage_one_kernel, rows, chips, heads),
        out_shape=(jax.ShapeDtypeStruct((tokens, wide + n_up * wide), bf), jax.ShapeDtypeStruct((chips, rows - 1, sub, patches, dim_local), bf), w2, w2),
        in_specs=[anyspec] + [vmspec] * 4 + [anyspec] * 4,
        out_specs=(anyspec,) * 4,
        scratch_shapes=[
            vm((tokens, dim), bf), vm((dim, n_w * wide), bf), vm((n_q, tokens, wide), bf), vm((2, patches, dim), bf),
            vm((2, sub * patches, wide), bf), vm((2, 2, sub * patches, wide // 2), bf), vm((2, patches, wide), bf), vm(b_up.shape, jnp.float32), vm(ln_scale.shape, jnp.float32),
            dma((3,)), dma((3,)), dma((rows - 1, 4)), dma((rows - 1, 4)), dma((2, rows)), dma((n_q + 1,)), dma, dma,
            dma((n_w,)), dma((n_w,)), dma((n_w,)), dma((n_w,)), dma((n_w + 1,)), dma((n_w + 1,)), dma((rows, n_w + 1)), dma((rows, n_w + 1)), dma((2,)), dma((2,)), dma((4,)), dma((4,)), dma((2, 2)),
        ],
        compiler_params=pltpu.CompilerParams(collective_id=0, has_side_effects=True, vmem_limit_bytes=VMEM_MAX),
        cost_estimate=pl.CostEstimate(flops=2 * tokens * dim * n_w * wide, bytes_accessed=1 << 27, transcendentals=0),
        name='stage_one',
    )(x_blk, ln_scale, qn_scale, kn_scale, b_up, wq, wu, w_o, w_down)
    return h, w2_own, w2_cross


def stage_two_kernel(rows, chips, x_hbm, h_hbm, w_o, w_down, w2_own, w2_cross, bias, out_hbm, h_v, w_v, ys_v, yt_v, x_v, rx_v, half_v, tot_v, t2_v, in_v, fin_v,
                     ld_sem, wa_send, wa_recv, wc_send, wc_recv, wd_send, wd_recv, wx_send, wx_recv, hf_send, hf_recv, x_send, x_recv, p_send, p_recv, t_send, t_recv,
                     i_send, i_recv, g_send, g_recv, s_send, s_recv, l_sem):
    p = Place(rows, chips)
    batch, patches, dim_local = x_hbm.shape
    sub = batch // (2 * CORES * chips)
    group = sub * patches
    ko, kd = w_o.shape[0], w_down.shape[0]
    cw = dim_local // CHUNKS
    far_rank = rows - 1

    def cols(c):
        return pl.ds(c * cw, cw)

    def two(c, slot, make):
        return [make(w_o.at[:, cols(c)], w_v.at[c, slot, pl.ds(0, ko), :], 0), make(w_down.at[:, cols(c)], w_v.at[c, slot, pl.ds(ko, kd), :], 1)]

    wa = [two(c, 1, lambda s, d, n, c=c: remote(s, d, wa_send.at[c, n], wa_recv.at[c, n], p.inner_peer)) for c in range(CHUNKS)]
    wc = [remote(w2_cross.at[:, cols(c)], w_v.at[c, 3], wc_send.at[c], wc_recv.at[c], p.inner_peer) for c in range(CHUNKS)]
    wd = [{r: remote(w_v.at[c, r], w_v.at[c, r], wd_send.at[c, r // 2], wd_recv.at[c, r // 2], p.sibling) for r in (1, 3)} for c in range(CHUNKS)]
    wx = [remote(w2_cross.at[:, cols(c)], w_v.at[c, 2], wx_send.at[c], wx_recv.at[c], p.sibling) for c in range(CHUNKS)]
    own_primary = [two(c, 0, lambda s, d, n, c=c: pltpu.make_async_copy(s, d, ld_sem.at[2 * c + n])) for c in range(CHUNKS)]
    own_other = [pltpu.make_async_copy(w2_own.at[:, cols(c)], w_v.at[c, 0], ld_sem.at[2 * c]) for c in range(CHUNKS)]
    cross_load = [pltpu.make_async_copy(w2_cross.at[:, cols(c)], w_v.at[c, 2], ld_sem.at[2 * CHUNKS + c]) for c in range(CHUNKS)]
    def h_copy(rank):
        return pltpu.make_async_copy(h_hbm.at[aligned(rank, group), :], h_v.at[aligned(rank, group), :], ld_sem.at[5 * CHUNKS + rank])


    def images(side, dx):
        return p.first_image(p.half if side == 0 else 1 - p.half, dx, p.core, batch)

    fin_load = [
        [pltpu.make_async_copy(x_hbm.at[pl.ds(images(side, 0), sub), :, cols(c)], fin_v.at[side, c], ld_sem.at[3 * CHUNKS + side * CHUNKS + c]) for c in range(CHUNKS)]
        for side in (0, 1)
    ]

    def p_copy(c, rank):
        return remote(ys_v.at[c, rank], yt_v.at[c, rank], p_send.at[c, rank], p_recv.at[c, rank], p.cross_peer)

    def half_copy(u, k):
        who = p.right_peer if k == 0 else p.left_peer
        return remote(x_v.at[u % 3, far_rank, k], half_v.at[u, k], hf_send.at[u, k], hf_recv.at[u, k], who)

    def x_copy(u, k):
        who = p.right_peer if k == 0 else p.left_peer
        return remote(x_v.at[u % 3, 2 - k], rx_v.at[u, k], x_send.at[u, k], x_recv.at[u, k], who)

    def t_copy(c):
        return remote(tot_v.at[1, c], t2_v.at[c], t_send.at[c], t_recv.at[c], p.cross_peer)

    def i_copy(c):
        return remote(tot_v.at[2, c], in_v.at[c], i_send.at[c], i_recv.at[c], p.inner_peer)

    def spot(side, dx, c, count=sub, first=0):
        return out_hbm.at[pl.ds(images(side, dx) + first, count), :, cols(c)]

    def g_copy(side, c, k):
        who = p.right_peer if k % 2 == 0 else p.left_peer
        if k < 2:
            src, dst = fin_v.at[side, c], spot(side, 0, c)
        else:
            src = dst = spot(side, chips - 1 if k == 2 else 1, c, 1, k - 2)
        return remote(src, dst, g_send.at[side, c, k], g_recv.at[side, c, k], who)

    def s_copy(side, c, k):
        here = spot(side, (0, chips - 1, 1, 2)[k], c)
        return remote(fin_v.at[side, c] if k == 0 else here, here, s_send.at[side, c, k], s_recv.at[side, c, k], p.sibling)

    def l_copy(side, c):
        return pltpu.make_async_copy(fin_v.at[side, c], spot(side, 0, c), l_sem.at[side, c])

    def add(a, b):
        return a.astype(jnp.float32) + b.astype(jnp.float32)

    def dot(rank, c, r):
        return jnp.dot(h_v[aligned(rank, group), :], w_v[c, r], preferred_element_type=jnp.float32).astype(jnp.bfloat16).reshape(sub, patches, cw)

    def received(c, r):
        if r == 2:

            @pl.when(p.primary)
            def _():
                cross_load[c].wait()

            @pl.when(jnp.logical_not(p.primary))
            def _():
                wx[c].wait_recv()

        elif r:

            @pl.when(jnp.logical_not(p.primary))
            def _():
                wd[c][r].wait_recv()

    def cross_part(c, r):
        received(c, r)

        def cell(n, carry):
            rank = far_rank - n
            ys_v[c, rank] = dot(rank, c, r)
            p_copy(c, rank).start()
            return carry

        lax.fori_loop(0, chips, cell, 0)

    def reuse(u):
        if u >= 3:
            for k in range(2):
                half_copy(u - 3, k).wait_send()
                x_copy(u - 3, k).wait_send()

    def mid_one(u, k):
        half_copy(u, k).wait_recv()
        s = u % 3
        x_v[s, 2 - k, k] = add(x_v[s, 2 - k, k], half_v[u, k]).astype(jnp.bfloat16)
        x_copy(u, k).start()

    def pair_part(u, c, r):
        reuse(u)
        s = u % 3
        received(c, r)

        def cell(n, carry):
            rank = far_rank - n
            part = dot(rank, c, r)
            p_copy(c, rank).wait_recv()
            x_v[s, rank] = add(part, yt_v[c, rank]).astype(jnp.bfloat16)

            @pl.when(n == 0)
            def _():
                half_copy(u, 0).start()
                half_copy(u, 1).start()

            for k in range(2):

                @pl.when(n == k + 1)
                def _(k=k):
                    mid_one(u, k)

            return carry

        lax.fori_loop(0, chips, cell, 0)

    def compute(u, c, r):
        reuse(u)
        s = u % 3
        received(c, r)

        def cell(n, carry):
            rank = far_rank - n
            if u == 0:
                h_copy(rank).wait()
            x_v[s, rank] = dot(rank, c, r)

            @pl.when(n == 0)
            def _():
                half_copy(u, 0).start()
                half_copy(u, 1).start()

            return carry

        lax.fori_loop(0, chips, cell, 0)

    def mid(u):
        mid_one(u, 0)
        mid_one(u, 1)

    def total(u, n):
        s = u % 3
        return add(x_v[s, 0, n], rx_v[u, 0, n]) + rx_v[u, 1, n].astype(jnp.float32)

    def arrived(u):
        x_copy(u, 0).wait_recv()
        x_copy(u, 1).wait_recv()

    def reduce(u, c, slot, send=None):
        arrived(u)
        for n in range(sub):
            tot_v[slot, c, n] = total(u, n).astype(jnp.bfloat16)
        if send is not None:
            send(c).start()

    def fetch_far(c):
        @pl.when(p.primary)
        def _():
            wc[c].wait_recv()
            wd[c][3].start()

    def fetch_inner(c):
        @pl.when(p.primary)
        def _():
            for copy in wa[c]:
                copy.wait_recv()
            wd[c][1].start()

    def pass_on(c):
        t_copy(c).wait_recv()
        for n in range(sub):
            tot_v[2, c, n] = add(tot_v[0, c, n], t2_v[c, n]).astype(jnp.bfloat16)
        i_copy(c).start()

    def home(side, c, u=None):
        if u is None:
            (i_copy if side else t_copy)(c).wait_recv()
        else:
            arrived(u)
        fin_load[side][c].wait()
        for n in range(sub):
            if u is not None:
                summed = total(u, n)
            else:
                summed = in_v[c, n].astype(jnp.float32) if side else add(tot_v[0, c, n], t2_v[c, n])
            fin_v[side, c, n] = (fin_v[side, c, n].astype(jnp.float32) + summed + bias[:, cols(c)]).astype(jnp.bfloat16)
        g_copy(side, c, 0).start()
        g_copy(side, c, 1).start()
        s_copy(side, c, 0).start()
        l_copy(side, c).start()

    def near(side, c):
        for k in range(2):
            g_copy(side, c, k).wait_recv()
            g_copy(side, c, 2 + k).start()
            s_copy(side, c, 1 + k).start()

    def far(side, c):
        g_copy(side, c, 2).wait_recv()
        g_copy(side, c, 3).wait_recv()
        s_copy(side, c, 3).start()

    def own_load(c, act):
        @pl.when(p.primary)
        def _():
            for copy in own_primary[c]:
                act(copy)

        @pl.when(jnp.logical_not(p.primary))
        def _():
            act(own_other[c])

    h_copy(far_rank).start()
    own_load(1, lambda copy: copy.start())
    for rank in reversed(range(far_rank)):
        h_copy(rank).start()
    own_load(0, lambda copy: copy.start())

    @pl.when(p.primary)
    def _():
        for c in reversed(range(CHUNKS)):
            cross_load[c].start()

    for side in (0, 1):
        for c in range(CHUNKS):
            fin_load[side][c].start()
    p.enter()

    @pl.when(p.primary)
    def _():
        for copy in [wx[1], wx[0]] + wc + wa[0] + wa[1]:
            copy.start()

    own_load(1, lambda copy: copy.wait())
    compute(0, 1, 0)
    compute(1, 1, 2)
    mid(0)
    cross_part(0, 2)
    mid(1)
    fetch_far(0)
    reduce(0, 1, 0)
    compute(2, 0, 3)
    reduce(1, 1, 1, t_copy)
    own_load(0, lambda copy: copy.wait())
    pair_part(3, 0, 0)
    mid(2)
    home(0, 0, 3)
    fetch_far(1)
    cross_part(1, 3)
    home(0, 1)
    fetch_inner(0)
    compute(4, 0, 1)
    near(0, 0)
    reduce(2, 0, 1, t_copy)
    mid(4)
    fetch_inner(1)
    pair_part(5, 1, 1)
    reduce(4, 0, 0)
    near(0, 1)
    pass_on(0)
    reduce(5, 1, 2, i_copy)
    home(1, 0)
    home(1, 1)
    far(0, 0)
    far(0, 1)
    near(1, 0)
    near(1, 1)
    far(1, 0)
    far(1, 1)

    for c in range(CHUNKS):
        for side in (0, 1):
            for k in range(4):
                s_copy(side, c, k).wait_recv()
                s_copy(side, c, k).wait_send()
                g_copy(side, c, k).wait_send()
            l_copy(side, c).wait()
        t_copy(c).wait_send()
        i_copy(c).wait_send()
        for rank in range(chips):
            p_copy(c, rank).wait_send()
    for u in (3, 4, 5):
        for k in range(2):
            half_copy(u, k).wait_send()
            x_copy(u, k).wait_send()

    @pl.when(p.primary)
    def _():
        for c in range(CHUNKS):
            wc[c].wait_send()
            wx[c].wait_send()
            for copy in wa[c]:
                copy.wait_send()
            for r in (1, 3):
                wd[c][r].wait_send()


def stage_two(rows, chips, x_blk, h, w_o, w_down, w2_own, w2_cross, b_out):
    batch, patches, dim_local = x_blk.shape
    sub = batch // (2 * CORES * chips)
    k_dim, cw = w2_own.shape[0], dim_local // CHUNKS
    units = 3 * CHUNKS
    bf, vm, dma = jnp.bfloat16, pltpu.VMEM, pltpu.SemaphoreType.DMA
    piece = (sub, patches, cw)
    anyspec, vmspec = pl.BlockSpec(memory_space=pl.ANY), pl.BlockSpec(memory_space=pltpu.VMEM)
    return pl.pallas_call(
        functools.partial(stage_two_kernel, rows, chips),
        out_shape=jax.ShapeDtypeStruct(x_blk.shape, bf),
        in_specs=[anyspec] * 6 + [vmspec],
        out_specs=anyspec,
        scratch_shapes=[
            vm(h.shape, bf), vm((CHUNKS, rows, k_dim, cw), bf), vm((CHUNKS, chips) + piece, bf), vm((CHUNKS, chips) + piece, bf), vm((3, chips) + piece, bf),
            vm((units, 2) + piece, bf), vm((units, 2, patches, cw), bf), vm((3, CHUNKS) + piece, bf), vm((CHUNKS,) + piece, bf), vm((CHUNKS,) + piece, bf),
            vm((2, CHUNKS) + piece, bf),
            dma((5 * CHUNKS + rows,)), dma((CHUNKS, 2)), dma((CHUNKS, 2)), dma((CHUNKS,)), dma((CHUNKS,)), dma((CHUNKS, 2)), dma((CHUNKS, 2)), dma((CHUNKS,)), dma((CHUNKS,)),
            dma((units, 2)), dma((units, 2)), dma((units, 2)), dma((units, 2)), dma((CHUNKS, chips)), dma((CHUNKS, chips)), dma((CHUNKS,)), dma((CHUNKS,)),
            dma((CHUNKS,)), dma((CHUNKS,)), dma((2, CHUNKS, 4)), dma((2, CHUNKS, 4)), dma((2, CHUNKS, 4)), dma((2, CHUNKS, 4)), dma((2, CHUNKS)),
        ],
        compiler_params=pltpu.CompilerParams(collective_id=1, has_side_effects=True, vmem_limit_bytes=VMEM_MAX),
        cost_estimate=pl.CostEstimate(flops=2 * h.shape[0] * k_dim * dim_local * rows, bytes_accessed=1 << 27, transcendentals=0),
        name='stage_two',
    )(x_blk, h, w_o, w_down, w2_own, w2_cross, b_out.reshape(1, dim_local))


def copy_kernel(src, dst, held, in_sem, out_sem):
    count = in_sem.shape[0]
    step = src.shape[0] // count
    loads = [pltpu.make_async_copy(src.at[pl.ds(n * step, step)], held.at[pl.ds(n * step, step)], in_sem.at[n]) for n in range(count)]
    stores = [pltpu.make_async_copy(held.at[pl.ds(n * step, step)], dst.at[pl.ds(n * step, step)], out_sem.at[n]) for n in range(count)]
    for c in loads:
        c.start()
    for n in range(count):
        loads[n].wait()
        stores[n].start()
    for c in stores:
        c.wait()


def copy_out(array):
    count = 16
    return pl.pallas_call(
        copy_kernel,
        out_shape=jax.ShapeDtypeStruct(array.shape, array.dtype),
        in_specs=[pl.BlockSpec(memory_space=pl.ANY)],
        out_specs=pl.BlockSpec(memory_space=pl.ANY),
        scratch_shapes=[pltpu.VMEM(array.shape, array.dtype), pltpu.SemaphoreType.DMA((count,)), pltpu.SemaphoreType.DMA((count,))],
        compiler_params=pltpu.CompilerParams(vmem_limit_bytes=VMEM_MAX),
        name='copy_out',
    )(array)


def solution(mesh):
    rows, cols = mesh.shape['m1'], mesh.shape['m2']
    chips = cols // CORES
    assert rows == 4 and chips == 4

    def local_layer(x_blk, ln_scale, qn_scale, kn_scale, w_qkv, w_up, b_up, w_o, w_down, b_out):
        h, w2_own, w2_cross = stage_one(
            rows, chips, x_blk, ln_scale[None], qn_scale[None], kn_scale[None], b_up[None], w_qkv.transpose(1, 0, 2), w_up, w_o, w_down
        )
        return copy_out(stage_two(rows, chips, x_blk, h, w_o, w_down, w2_own, w2_cross, b_out))

    return jax.shard_map(local_layer, mesh=mesh, in_specs=(P('dp', None, 'm1'), P(), P(), P(), P('m1', None, 'm2'), P('m1', 'm2'), P('m2'), P('m2', 'm1'), P('m2', 'm1'), P('m1')), out_specs=P('dp', None, 'm1'), check_vma=False)
```

```python
import functools

import jax
import jax.numpy as jnp
from jax import lax
from jax.experimental import pallas as pl
from jax.experimental.pallas import tpu as pltpu
from jax.sharding import PartitionSpec as P

LN_EPS = 1e-6
CORES = 2
LINES = 16
LANES = 128
NEXT_CHUNK = (2, 3, 4, None, 5, 6, None)
CHUNKS = 4
X_SLOTS = 6
SEND_SLOTS = 3
PLAN = (
    ('send', 1, 2), ('part', 3, 2, 0), ('part', 2, 0, 1), ('mid', 0), ('mid', 1), ('part', 3, 0, 2), ('sum', 3, 2, 0), ('pass', 2, 3),
    ('send', 0, 2), ('pair', 1, 0, 3), ('sum', 2, 0, 1), ('mid', 2), ('part', 2, 2, 4), ('send', 2, 3), ('sum', 3, 0, 2), ('home', 0, 3),
    ('pair', 0, 0, 5), ('mid', 4), ('pass', 2, 1), ('home', 0, 0, 5), ('pass', 0, 3), ('send', 0, 3), ('pair', 2, 1, 6), ('pass', 1, 3),
    ('near', 0, 0), ('home', 0, 1, 3), ('pass', 3, 3), ('pass', 0, 1), ('sum', 2, 1, 6), ('sum', 2, 2, 4), ('send', 3, 3), ('near', 0, 3),
    ('pair', 0, 1, 7), ('pass', 3, 1), ('home', 0, 2), ('far', 0, 0), ('sum', 0, 1, 7), ('far', 0, 3), ('near', 0, 1), ('send', 1, 3),
    ('pass', 1, 1), ('near', 0, 2), ('pair', 3, 1, 8), ('home', 1, 0), ('far', 0, 1), ('sum', 3, 1, 8), ('far', 0, 2), ('home', 1, 2),
    ('pair', 1, 1, 9), ('near', 1, 2), ('near', 1, 0), ('sum', 1, 1, 9), ('home', 1, 3), ('home', 1, 1), ('near', 1, 3), ('near', 1, 1),
    ('far', 1, 3), ('far', 1, 0), ('far', 1, 2), ('far', 1, 1),
)
INNER_ORDER = ((2, 3), (1, 3), (0, 3), (2, 1), (3, 3), (0, 1), (3, 1), (1, 1))
VMEM_MAX = 67043328
MESH = pl.DeviceIdType.MESH


def layer_norm(values, scale):
    mean = jnp.mean(values, axis=-1, keepdims=True)
    centered = values - mean
    variance = jnp.mean(centered * centered, axis=-1, keepdims=True)
    return centered * lax.rsqrt(variance + LN_EPS) * scale


class Place:
    def __init__(self, rows, chips):
        self.rows, self.chips = rows, chips
        self.dp, self.row = lax.axis_index('dp'), lax.axis_index('m1')
        col = lax.axis_index('m2')
        self.col, self.chip, self.core = col, col // CORES, lax.rem(col, CORES)
        self.inner = self.row + 1 - 2 * lax.rem(self.row, 2)
        self.cross = rows - 1 - self.row
        self.pair = self.row // 2
        self.half = lax.rem((self.row + 1) // 2, 2)
        self.primary = self.core == self.pair
        self.inner_peer = (self.dp, self.inner, col)
        self.cross_peer = (self.dp, self.cross, col)
        self.right_peer = (self.dp, self.row, self.at(1) * CORES + self.core)
        self.left_peer = (self.dp, self.row, self.at(chips - 1) * CORES + self.core)
        self.sibling = (self.dp, self.row, self.chip * CORES + 1 - self.core)

    def at(self, dx):
        return lax.rem(self.chip + dx, self.chips)

    def enter(self):
        barrier = pltpu.get_barrier_semaphore()
        partners = (self.inner_peer, self.cross_peer, self.right_peer, self.left_peer, self.sibling)
        for who in partners:
            pl.semaphore_signal(barrier, inc=1, device_id=who, device_id_type=MESH)
        pl.semaphore_wait(barrier, len(partners))

    def first_image(self, half, dx, core, batch):
        per = batch // (2 * CORES)
        return (half * CORES + core) * per + self.at(dx) * (per // self.chips)


def remote(src, dst, ssem, rsem, who):
    return pltpu.make_async_remote_copy(src_ref=src, dst_ref=dst, send_sem=ssem, recv_sem=rsem, device_id=who, device_id_type=MESH)


def aligned(index, size):
    return pl.ds(pl.multiple_of(index * size, size), size)


def stage_one_kernel(rows, chips, heads, x_hbm, ln_all, qn_scale, kn_scale, bias_own, wq, wu, w_o, w_down, h_hbm, raw, w2_own, w2_cross, u_v, w_v, qkv_v, st_v, up_v, last_v, at_v, bias_v, ln_scale,
                     xs_send, xs_recv, ag_send, ag_recv, ld_sem, own_sem, b_send, b_recv, wa_send, wa_recv, wb_send, wb_recv, wc_send, wc_recv,
                     wd_send, wd_recv, up_sem, at_sem, v_send, v_recv, last_sem):
    p = Place(rows, chips)
    batch, patches, dim_local = x_hbm.shape
    dim = dim_local * rows
    wide = wq.shape[2]
    head_dim = wide // heads
    n_q, n_up = wq.shape[0], wu.shape[1] // wide
    n_w = n_q + n_up
    sub = batch // (2 * CORES * chips)
    group = sub * patches
    dx_of = (0, chips - 1, 1, 2)

    xa = remote(x_hbm.at[pl.ds(p.first_image(p.half, 0, p.core, batch), sub)], raw.at[0, 1], xs_send.at[0], xs_recv.at[0], p.cross_peer)
    xb = remote(x_hbm.at[pl.ds(p.first_image(1 - p.half, 0, p.core, batch), sub)], raw.at[0, 0], xs_send.at[1], xs_recv.at[1], p.inner_peer)
    xc = remote(raw.at[0, 0], raw.at[0, 2], xs_send.at[2], xs_recv.at[2], p.cross_peer)

    def ag(e, k):
        src, dst = ((raw.at[0, e], raw.at[1, e]), (raw.at[0, e], raw.at[2, e]), (raw.at[1, e, 0], raw.at[3, e, 0]), (raw.at[2, e, 1], raw.at[3, e, 1]))[k]
        return remote(src, dst, ag_send.at[e, k], ag_recv.at[e, k], p.right_peer if k % 2 == 0 else p.left_peer)

    def block(r, k):
        return w_v.at[pl.ds(r * dim_local, dim_local), aligned(k, wide)]

    def from_own(k, make, act):
        @pl.when(k < n_q)
        def _():
            act(make(wq.at[jnp.minimum(k, n_q - 1)]))

        @pl.when(k >= n_q)
        def _():
            act(make(wu.at[:, aligned(jnp.maximum(k - n_q, 0), wide)]))

    def wa(k, src=None):
        return remote(block(1, k) if src is None else src, block(1, k), wa_send.at[k], wa_recv.at[k], p.inner_peer)

    def wb(k, src=None):
        return remote(block(2, k) if src is None else src, block(2, k), wb_send.at[k], wb_recv.at[k], p.cross_peer)

    def wc(k):
        return remote(block(2, k), block(3, k), wc_send.at[k], wc_recv.at[k], p.inner_peer)

    def wd(r, k, src=None):
        return remote(block(r, k) if src is None else src, block(r, k), wd_send.at[r, k], wd_recv.at[r, k], p.sibling)

    own_copies = [pltpu.make_async_copy(wq.at[k], block(0, k), own_sem.at[k]) for k in range(n_q)]
    own_copies.append(pltpu.make_async_copy(wu, w_v.at[pl.ds(0, dim_local), pl.ds(n_q * wide, n_up * wide)], own_sem.at[n_q]))
    bias_copy = remote(bias_own, bias_v, b_send, b_recv, p.sibling)

    ko, kd = w_o.shape[0], w_down.shape[0]

    def two(dst, n, who):
        return [remote(w_o, dst.at[pl.ds(0, ko), :], v_send.at[n], v_recv.at[n], who), remote(w_down, dst.at[pl.ds(ko, kd), :], v_send.at[n + 1], v_recv.at[n + 1], who)]

    v_own, v_cross = two(w2_own, 0, p.sibling), two(w2_cross, 2, p.cross_peer)

    for r, source in enumerate((p.row, p.inner, p.cross, lax.rem(p.row + 2, rows))):
        ln_scale[:, r * dim_local : (r + 1) * dim_local] = ln_all[:, aligned(source, dim_local)]

    def start(copy):
        copy.start()

    def pump(k):
        @pl.when(p.primary)
        def _():
            wb(k).wait_recv()
            for c in wc_last if k == n_w - 1 else [wc(k)]:
                c.start()
            wd(2, k).start()
            later = NEXT_CHUNK[k]
            if later is not None:
                from_own(later, functools.partial(wa, later), start)
                from_own(later, functools.partial(wd, 0, later), start)

    def last_half(r, n):
        return w_v.at[pl.ds(r * dim_local, dim_local), pl.ds((n_w - 1) * wide + n * (wide // 2), wide // 2)]

    wc_last = [remote(last_half(2, n), last_half(3, n), wc_send.at[n_w - 1 + n], wc_recv.at[n_w - 1 + n], p.inner_peer) for n in range(2)]
    wd_last = [remote(last_half(3, n), last_half(3, n), wd_send.at[n, n_w], wd_recv.at[n, n_w], p.sibling) for n in range(2)]

    def hand_over(k):
        @pl.when(p.primary)
        def _():
            wa(k).wait_recv()
            wd(1, k).start()
            wc(k).wait_recv()
            wd(3, k).start()

    def receive(k):
        @pl.when(jnp.logical_not(p.primary))
        def _():
            for r in range(rows):
                wd(r, k).wait_recv()

    def load_copies(rank_dx, rank, s, b):
        image = p.first_image(p.half, rank_dx, p.core, batch) + s
        yield pltpu.make_async_copy(x_hbm.at[image], st_v.at[b, :, pl.ds(0, dim_local)], ld_sem.at[b, 0])
        for e in range(rows - 1):
            yield pltpu.make_async_copy(raw.at[rank, e, s], st_v.at[b, :, pl.ds((e + 1) * dim_local, dim_local)], ld_sem.at[b, e + 1])

    def normalize(ranks):
        jobs = [(rank, s) for rank in ranks for s in range(sub)]
        loads = [list(load_copies(dx_of[rank], rank, s, n % 2)) for n, (rank, s) in enumerate(jobs)]
        for n in range(len(jobs)):
            if n == 0:
                for c in loads[0]:
                    c.start()
            if n + 1 < len(jobs):
                for c in loads[n + 1]:
                    c.start()
            for c in loads[n]:
                c.wait()
            rank, s = jobs[n]

            def lines(m, carry, b=n % 2, base=(rank * sub + s) * patches):
                here = aligned(m, LINES)
                to = pl.ds(pl.multiple_of(base + m * LINES, LINES), LINES)
                parts = [slice(j * LANES, (j + 1) * LANES) for j in range(dim // LANES)]

                def load(part):
                    return st_v[b, here, part].astype(jnp.float32)

                mean = jnp.sum(functools.reduce(jnp.add, [load(part) for part in parts]), axis=-1, keepdims=True) / dim
                squares = [(load(part) - mean) * (load(part) - mean) for part in parts]
                inverse = lax.rsqrt(jnp.sum(functools.reduce(jnp.add, squares), axis=-1, keepdims=True) / dim + LN_EPS)
                for part in parts:
                    u_v[to, part] = ((load(part) - mean) * inverse * ln_scale[:, part]).astype(jnp.bfloat16)
                return carry

            lax.fori_loop(0, patches // LINES, lines, 0, unroll=4)

    def dot_cell(rank, k):
        return jnp.dot(u_v[aligned(rank, group), :], w_v[:, aligned(k, wide)], preferred_element_type=jnp.float32).astype(jnp.bfloat16)

    def qkv_cell(rank, k):
        z = dot_cell(rank, k)
        to = aligned(rank, group)

        @pl.when(k == n_q - 1)
        def _():
            qkv_v[k, to, :] = z

        @pl.when(k < n_q - 1)
        def _():
            scale = jnp.where(k == 0, qn_scale[...], kn_scale[...])
            for hd in range(heads):
                part = slice(hd * head_dim, (hd + 1) * head_dim)
                qkv_v[k, to, part] = layer_norm(z[:, part].astype(jnp.float32), scale).astype(jnp.bfloat16)

    def at_copy(image, b):
        return pltpu.make_async_copy(at_v.at[b], h_hbm.at[aligned(image, patches), pl.ds(0, wide)], at_sem.at[b])

    def attend(first, count):
        def one(image, carry):
            b = lax.rem(image, 2)
            here = aligned(image, patches)

            @pl.when(image >= 2)
            def _():
                at_copy(image - 2, b).wait()

            for hd in range(heads):
                part = slice(hd * head_dim, (hd + 1) * head_dim)
                q, k, v = (qkv_v[n, here, part] for n in range(3))
                scores = lax.dot_general(q, k, (((1,), (1,)), ((), ())), preferred_element_type=jnp.float32) * head_dim ** -0.5
                probs = jnp.exp(scores - jnp.max(scores, axis=-1, keepdims=True))
                probs = (probs / jnp.sum(probs, axis=-1, keepdims=True)).astype(jnp.bfloat16)
                at_v[b, :, part] = jnp.dot(probs, v, preferred_element_type=jnp.float32).astype(jnp.bfloat16)
            at_copy(image, b).start()
            return carry

        lax.fori_loop(first, first + count, one, 0)

    def up_copy(rank, k, b):
        return pltpu.make_async_copy(up_v.at[b], h_hbm.at[aligned(rank, group), aligned(k - n_q + 1, wide)], up_sem.at[b])

    def bias_of(here):
        return jnp.where(p.primary, bias_own[:, here], bias_v[:, here])

    def up_chunk(k, carry):
        hand_over(k)
        receive(k)
        bias = bias_of(aligned(k - n_q, wide))

        def cell(rank, carry):
            b = lax.rem(rank, 2)

            @pl.when(jnp.logical_or(k > n_q, rank >= 2))
            def _():
                up_copy(rank, k, b).wait()

            m = dot_cell(rank, k).astype(jnp.float32) + bias
            up_v[b] = (0.5 * m * (1.0 + lax.erf(m * 0.5 ** 0.5))).astype(jnp.bfloat16)
            up_copy(rank, k, b).start()
            return carry

        return lax.fori_loop(0, rows, cell, carry)

    def last_copy(rank, n):
        to = pl.ds(wide + (n_up - 1) * wide + n * (wide // 2), wide // 2)
        return pltpu.make_async_copy(last_v.at[n, lax.rem(rank, 2)], h_hbm.at[aligned(rank, group), to], last_sem.at[n, lax.rem(rank, 2)])

    def last_chunk(n):
        @pl.when(p.primary)
        def _():
            if n == 0:
                wa(n_w - 1).wait_recv()
                wd(1, n_w - 1).start()
            wc_last[n].wait_recv()
            wd_last[n].start()

        @pl.when(jnp.logical_not(p.primary))
        def _():
            if n == 0:
                for r in range(rows - 1):
                    wd(r, n_w - 1).wait_recv()
            wd_last[n].wait_recv()

        first = (n_up - 1) * wide + n * (wide // 2)
        bias = bias_of(pl.ds(first, wide // 2))
        weight = pl.ds(n_q * wide + first, wide // 2)

        def cell(rank, carry):
            @pl.when(rank >= 2)
            def _():
                last_copy(rank - 2, n).wait()

            m = jnp.dot(u_v[aligned(rank, group), :], w_v[:, weight], preferred_element_type=jnp.float32).astype(jnp.bfloat16).astype(jnp.float32) + bias
            last_v[n, lax.rem(rank, 2)] = (0.5 * m * (1.0 + lax.erf(m * 0.5 ** 0.5))).astype(jnp.bfloat16)
            last_copy(rank, n).start()
            return carry

        lax.fori_loop(0, rows, cell, 0)

    p.enter()
    xb.start()

    @pl.when(jnp.logical_not(p.primary))
    def _():
        from_own(0, functools.partial(wb, 0), start)

    xa.start()
    bias_copy.start()

    @pl.when(p.primary)
    def _():
        for c in own_copies:
            c.start()
        for k in range(NEXT_CHUNK[0]):
            from_own(k, functools.partial(wa, k), start)
            from_own(k, functools.partial(wd, 0, k), start)

    xb.wait_recv()
    xc.start()
    ag(0, 0).start()
    ag(0, 1).start()

    @pl.when(jnp.logical_not(p.primary))
    def _():
        for k in range(1, n_w):
            from_own(k, functools.partial(wb, k), start)
        for c in v_cross:
            c.start()

    xa.wait_recv()
    ag(1, 0).start()
    ag(1, 1).start()
    pump(0)
    xc.wait_recv()
    ag(2, 0).start()
    ag(2, 1).start()
    normalize((0,))

    def forward(e):
        for k in range(2):
            ag(e, k).wait_recv()
            ag(e, 2 + k).start()

    @pl.when(p.primary)
    def _():
        for c in own_copies:
            c.wait()
        for c in v_own:
            c.start()

    def cells(count, job):
        def cell(n, carry):
            qkv_cell(*job(n))
            return carry

        lax.fori_loop(0, count, cell, 0)

    forward(0)
    hand_over(0)
    pump(1)
    forward(1)
    receive(0)
    cells(1, lambda n: (n, n))
    hand_over(1)
    pump(2)
    receive(1)
    cells(1, lambda n: (n, n + 1))
    forward(2)
    normalize((1, 2))
    hand_over(2)
    pump(3)
    receive(2)
    early = (n_q - 1) * 2
    cells(early + rows - 1, lambda n: (jnp.where(n < early, 1 + lax.rem(n, 2), n - early), jnp.where(n < early, n // 2, n_q - 1)))
    pump(4)
    attend(0, (rows - 1) * sub)
    pump(5)
    for e in range(rows - 1):
        ag(e, 2).wait_recv()
        ag(e, 3).wait_recv()
    normalize((rows - 1,))
    cells(n_q, lambda n: (rows - 1, n))
    pump(6)
    attend((rows - 1) * sub, sub)
    bias_copy.wait_recv()
    lax.fori_loop(n_q, n_w - 1, up_chunk, 0)
    last_chunk(0)
    last_chunk(1)

    for b in range(2):
        at_copy(b, b).wait()
        up_copy(b, n_q, b).wait()
        for n in range(2):
            last_copy(b, n).wait()
    for c in (xa, xb, xc, bias_copy):
        c.wait_send()
    for e in range(rows - 1):
        for k in range(4):
            ag(e, k).wait_send()

    @pl.when(p.primary)
    def _():
        for k in range(n_w):
            wa(k).wait_send()
            if k < n_w - 1:
                wc(k).wait_send()
            for r in range(rows if k < n_w - 1 else rows - 1):
                wd(r, k).wait_send()
        for c in v_own + wc_last + wd_last:
            c.wait_send()
        for c in v_cross:
            c.wait_recv()

    @pl.when(jnp.logical_not(p.primary))
    def _():
        for k in range(n_w):
            wb(k).wait_send()
        for c in v_cross:
            c.wait_send()
        for c in v_own:
            c.wait_recv()


def stage_one(rows, chips, x_blk, ln_scale, qn_scale, kn_scale, b_up, wq, wu, w_o, w_down):
    batch, patches, dim_local = x_blk.shape
    dim, wide = rows * dim_local, wq.shape[2]
    heads = wide // qn_scale.shape[1]
    n_q, n_up = wq.shape[0], wu.shape[1] // wide
    n_w = n_q + n_up
    sub = batch // (2 * CORES * chips)
    tokens = chips * sub * patches
    bf, vm, dma = jnp.bfloat16, pltpu.VMEM, pltpu.SemaphoreType.DMA
    anyspec, vmspec = pl.BlockSpec(memory_space=pl.ANY), pl.BlockSpec(memory_space=pltpu.VMEM)
    w2 = jax.ShapeDtypeStruct((w_o.shape[0] + w_down.shape[0], dim_local), bf)
    h, _, w2_own, w2_cross = pl.pallas_call(
        functools.partial(stage_one_kernel, rows, chips, heads),
        out_shape=(jax.ShapeDtypeStruct((tokens, wide + n_up * wide), bf), jax.ShapeDtypeStruct((chips, rows - 1, sub, patches, dim_local), bf), w2, w2),
        in_specs=[anyspec] + [vmspec] * 4 + [anyspec] * 4,
        out_specs=(anyspec,) * 4,
        scratch_shapes=[
            vm((tokens, dim), bf), vm((dim, n_w * wide), bf), vm((n_q, tokens, wide), bf), vm((2, patches, dim), bf),
            vm((2, sub * patches, wide), bf), vm((2, 2, sub * patches, wide // 2), bf), vm((2, patches, wide), bf), vm(b_up.shape, jnp.float32), vm(ln_scale.shape, jnp.float32),
            dma((3,)), dma((3,)), dma((rows - 1, 4)), dma((rows - 1, 4)), dma((2, rows)), dma((n_q + 1,)), dma, dma,
            dma((n_w,)), dma((n_w,)), dma((n_w,)), dma((n_w,)), dma((n_w + 1,)), dma((n_w + 1,)), dma((rows, n_w + 1)), dma((rows, n_w + 1)), dma((2,)), dma((2,)), dma((4,)), dma((4,)), dma((2, 2)),
        ],
        compiler_params=pltpu.CompilerParams(collective_id=0, has_side_effects=True, vmem_limit_bytes=VMEM_MAX),
        cost_estimate=pl.CostEstimate(flops=2 * tokens * dim * n_w * wide, bytes_accessed=1 << 27, transcendentals=0),
        name='stage_one',
    )(x_blk, ln_scale, qn_scale, kn_scale, b_up, wq, wu, w_o, w_down)
    return h, w2_own, w2_cross


def stage_two_kernel(rows, chips, x_hbm, h_hbm, w_o, w_down, w2_own, w2_cross, bias, out_hbm, h_v, w_v, ys_v, yt_v, x_v, rx_v, half_v, tot_v, t2_v, in_v, fin_v,
                     ld_sem, wa_send, wa_recv, wc_send, wc_recv, wd_send, wd_recv, wx_send, wx_recv, hf_send, hf_recv, x_send, x_recv, p_send, p_recv, t_send, t_recv,
                     i_send, i_recv, g_send, g_recv, s_send, s_recv, l_sem):
    p = Place(rows, chips)
    batch, patches, dim_local = x_hbm.shape
    sub = batch // (2 * CORES * chips)
    group = sub * patches
    ko, kd = w_o.shape[0], w_down.shape[0]
    cw = dim_local // CHUNKS
    far_rank = rows - 1
    sends = [step[1:] for step in PLAN if step[0] == 'send']
    units = [step for step in PLAN if step[0] in ('part', 'pair')]
    late = [step[1] for step in PLAN if step[0] == 'sum' and step[2] == 2]

    def cols(c):
        return pl.ds(c * cw, cw)

    def two(c, slot, make):
        return [make(w_o.at[:, cols(c)], w_v.at[c, slot, pl.ds(0, ko), :], 0), make(w_down.at[:, cols(c)], w_v.at[c, slot, pl.ds(ko, kd), :], 1)]

    wa = [two(c, 1, lambda s, d, n, c=c: remote(s, d, wa_send.at[c, n], wa_recv.at[c, n], p.inner_peer)) for c in range(CHUNKS)]
    wc = [remote(w2_cross.at[:, cols(c)], w_v.at[c, 3], wc_send.at[c], wc_recv.at[c], p.inner_peer) for c in range(CHUNKS)]
    wd = [{r: remote(w_v.at[c, r], w_v.at[c, r], wd_send.at[c, r // 2], wd_recv.at[c, r // 2], p.sibling) for r in (1, 3)} for c in range(CHUNKS)]
    wx = [remote(w2_cross.at[:, cols(c)], w_v.at[c, 2], wx_send.at[c], wx_recv.at[c], p.sibling) for c in range(CHUNKS)]
    own_primary = [two(c, 0, lambda s, d, n, c=c: pltpu.make_async_copy(s, d, ld_sem.at[2 * c + n])) for c in range(CHUNKS)]
    own_other = [pltpu.make_async_copy(w2_own.at[:, cols(c)], w_v.at[c, 0], ld_sem.at[2 * c]) for c in range(CHUNKS)]
    cross_load = [pltpu.make_async_copy(w2_cross.at[:, cols(c)], w_v.at[c, 2], ld_sem.at[2 * CHUNKS + c]) for c in range(CHUNKS)]
    def h_copy(rank):
        return pltpu.make_async_copy(h_hbm.at[aligned(rank, group), :], h_v.at[aligned(rank, group), :], ld_sem.at[5 * CHUNKS + rank])


    def images(side, dx):
        return p.first_image(p.half if side == 0 else 1 - p.half, dx, p.core, batch)

    fin_load = [
        [pltpu.make_async_copy(x_hbm.at[pl.ds(images(side, 0), sub), :, cols(c)], fin_v.at[side, c], ld_sem.at[3 * CHUNKS + side * CHUNKS + c]) for c in range(CHUNKS)]
        for side in (0, 1)
    ]

    def p_copy(n, rank):
        return remote(ys_v.at[n % SEND_SLOTS, rank], yt_v.at[n, rank], p_send.at[n, rank], p_recv.at[n, rank], p.cross_peer)

    def half_copy(u, k):
        who = p.right_peer if k == 0 else p.left_peer
        return remote(x_v.at[u % X_SLOTS, far_rank, k], half_v.at[u, k], hf_send.at[u, k], hf_recv.at[u, k], who)

    def x_copy(u, k):
        who = p.right_peer if k == 0 else p.left_peer
        return remote(x_v.at[u % X_SLOTS, 2 - k], rx_v.at[u, k], x_send.at[u, k], x_recv.at[u, k], who)

    def t_copy(c):
        return remote(tot_v.at[1, c], t2_v.at[c], t_send.at[c], t_recv.at[c], p.cross_peer)

    def i_copy(c):
        return remote(tot_v.at[2, c], in_v.at[c], i_send.at[c], i_recv.at[c], p.inner_peer)

    def spot(side, dx, c, count=sub, first=0):
        return out_hbm.at[pl.ds(images(side, dx) + first, count), :, cols(c)]

    def g_copy(side, c, k):
        who = p.right_peer if k % 2 == 0 else p.left_peer
        if k < 2:
            src, dst = fin_v.at[side, c], spot(side, 0, c)
        else:
            src = dst = spot(side, chips - 1 if k == 2 else 1, c, 1, k - 2)
        return remote(src, dst, g_send.at[side, c, k], g_recv.at[side, c, k], who)

    def s_copy(side, c, k):
        here = spot(side, (0, chips - 1, 1, 2)[k], c)
        return remote(fin_v.at[side, c] if k == 0 else here, here, s_send.at[side, c, k], s_recv.at[side, c, k], p.sibling)

    def l_copy(side, c):
        return pltpu.make_async_copy(fin_v.at[side, c], spot(side, 0, c), l_sem.at[side, c])

    def add(a, b):
        return a.astype(jnp.float32) + b.astype(jnp.float32)

    def dot(rank, c, r):
        return jnp.dot(h_v[aligned(rank, group), :], w_v[c, r], preferred_element_type=jnp.float32).astype(jnp.bfloat16).reshape(sub, patches, cw)

    def own_load(c, act):
        @pl.when(p.primary)
        def _():
            for copy in own_primary[c]:
                act(copy)

        @pl.when(jnp.logical_not(p.primary))
        def _():
            act(own_other[c])

    def received(c, r):
        if r == 0:
            own_load(c, lambda copy: copy.wait())
        elif r == 2:

            @pl.when(p.primary)
            def _():
                cross_load[c].wait()

            @pl.when(jnp.logical_not(p.primary))
            def _():
                wx[c].wait_recv()

        elif r:

            @pl.when(jnp.logical_not(p.primary))
            def _():
                wd[c][r].wait_recv()

    def cross_part(c, r):
        received(c, r)
        number = sends.index((c, r))
        if number >= SEND_SLOTS:
            for rank in range(chips):
                p_copy(number - SEND_SLOTS, rank).wait_send()

        def cell(n, carry):
            rank = far_rank - n
            if number == 0:
                h_copy(rank).wait()
            ys_v[number % SEND_SLOTS, rank] = dot(rank, c, r)
            p_copy(number, rank).start()
            return carry

        lax.fori_loop(0, chips, cell, 0)

    def reuse(u):
        if u >= X_SLOTS:
            for k in range(2):
                half_copy(u - X_SLOTS, k).wait_send()
                x_copy(u - X_SLOTS, k).wait_send()

    def mid_one(u, k):
        half_copy(u, k).wait_recv()
        s = u % X_SLOTS
        x_v[s, 2 - k, k] = add(x_v[s, 2 - k, k], half_v[u, k]).astype(jnp.bfloat16)
        x_copy(u, k).start()

    def pair_part(u, c, r):
        reuse(u)
        s = u % X_SLOTS
        received(c, r)
        number = sends.index((c, r + 2))

        def cell(n, carry):
            rank = far_rank - n
            part = dot(rank, c, r)
            p_copy(number, rank).wait_recv()
            x_v[s, rank] = add(part, yt_v[number, rank]).astype(jnp.bfloat16)

            @pl.when(n == 0)
            def _():
                half_copy(u, 0).start()
                half_copy(u, 1).start()

            for k in range(2):

                @pl.when(n == k + 1)
                def _(k=k):
                    mid_one(u, k)

            return carry

        lax.fori_loop(0, chips, cell, 0)

    def compute(u, c, r):
        reuse(u)
        s = u % X_SLOTS
        received(c, r)

        def cell(n, carry):
            rank = far_rank - n
            x_v[s, rank] = dot(rank, c, r)

            @pl.when(n == 0)
            def _():
                half_copy(u, 0).start()
                half_copy(u, 1).start()

            return carry

        lax.fori_loop(0, chips, cell, 0)

    def mid(u):
        mid_one(u, 0)
        mid_one(u, 1)

    def total(u, n):
        s = u % X_SLOTS
        return add(x_v[s, 0, n], rx_v[u, 0, n]) + rx_v[u, 1, n].astype(jnp.float32)

    def arrived(u):
        x_copy(u, 0).wait_recv()
        x_copy(u, 1).wait_recv()

    def reduce(u, c, slot, send=None):
        arrived(u)
        for n in range(sub):
            tot_v[slot, c, n] = total(u, n).astype(jnp.bfloat16)
        if send is not None:
            send(c).start()

    def fetch_far(c):
        @pl.when(p.primary)
        def _():
            wc[c].wait_recv()
            wd[c][3].start()

    def fetch_inner(c):
        @pl.when(p.primary)
        def _():
            for copy in wa[c]:
                copy.wait_recv()
            wd[c][1].start()

    def home(side, c, u=None):
        if u is None:
            (i_copy if side else t_copy)(c).wait_recv()
        else:
            arrived(u)
        fin_load[side][c].wait()
        for n in range(sub):
            if u is not None:
                summed = total(u, n)
            else:
                summed = in_v[c, n].astype(jnp.float32) if side else add(tot_v[0, c, n], t2_v[c, n])
            fin_v[side, c, n] = (fin_v[side, c, n].astype(jnp.float32) + summed + bias[:, cols(c)]).astype(jnp.bfloat16)
        g_copy(side, c, 0).start()
        g_copy(side, c, 1).start()
        s_copy(side, c, 0).start()
        l_copy(side, c).start()

    def near(side, c):
        for k in range(2):
            g_copy(side, c, k).wait_recv()
            g_copy(side, c, 2 + k).start()
            s_copy(side, c, 1 + k).start()

    def far(side, c):
        g_copy(side, c, 2).wait_recv()
        g_copy(side, c, 3).wait_recv()
        s_copy(side, c, 3).start()

    for rank in reversed(range(chips)):
        h_copy(rank).start()
    needs = [step[1:3] for step in PLAN if step[0] in ('send', 'part', 'pair')]
    for c, r in needs:
        if r == 0:
            own_load(c, lambda copy: copy.start())
        elif r == 2:

            @pl.when(p.primary)
            def _(c=c):
                cross_load[c].start()

    for side in (0, 1):
        for c in range(CHUNKS):
            fin_load[side][c].start()
    p.enter()

    @pl.when(p.primary)
    def _():
        for c, r in needs:
            if r == 2:
                wx[c].start()
        for c, r in INNER_ORDER:
            for copy in [wc[c]] if r == 3 else wa[c]:
                copy.start()

    assert PLAN[0][0] == 'send'
    for step, *of in PLAN:
        if step == 'send':
            cross_part(*of)
        elif step == 'part':
            compute(of[2], of[0], of[1])
        elif step == 'pair':
            pair_part(of[2], of[0], of[1])
        elif step == 'mid':
            mid(*of)
        elif step == 'sum':
            c, r, u = of
            reduce(u, c, {0: 0, 2: 1, 1: 2}[r], {0: None, 2: t_copy, 1: i_copy}[r])
        elif step == 'pass':
            (fetch_far if of[1] == 3 else fetch_inner)(of[0])
        elif step == 'home':
            home(*of)
        elif step == 'near':
            near(*of)
        else:
            far(*of)

    for c in range(CHUNKS):
        for side in (0, 1):
            for k in range(4):
                s_copy(side, c, k).wait_recv()
                s_copy(side, c, k).wait_send()
                g_copy(side, c, k).wait_send()
            l_copy(side, c).wait()
        if c in late:
            t_copy(c).wait_send()
        i_copy(c).wait_send()
    for number in range(len(sends) - SEND_SLOTS, len(sends)):
        for rank in range(chips):
            p_copy(number, rank).wait_send()
    for u in range(len(units) - X_SLOTS, len(units)):
        for k in range(2):
            half_copy(u, k).wait_send()
            x_copy(u, k).wait_send()

    @pl.when(p.primary)
    def _():
        for c in range(CHUNKS):
            wc[c].wait_send()
            wx[c].wait_send()
            for copy in wa[c]:
                copy.wait_send()
            for r in (1, 3):
                wd[c][r].wait_send()


def stage_two(rows, chips, x_blk, h, w_o, w_down, w2_own, w2_cross, b_out):
    batch, patches, dim_local = x_blk.shape
    sub = batch // (2 * CORES * chips)
    k_dim, cw = w2_own.shape[0], dim_local // CHUNKS
    units = sum(step[0] in ('part', 'pair') for step in PLAN)
    sends = sum(step[0] == 'send' for step in PLAN)
    bf, vm, dma = jnp.bfloat16, pltpu.VMEM, pltpu.SemaphoreType.DMA
    piece = (sub, patches, cw)
    anyspec, vmspec = pl.BlockSpec(memory_space=pl.ANY), pl.BlockSpec(memory_space=pltpu.VMEM)
    return pl.pallas_call(
        functools.partial(stage_two_kernel, rows, chips),
        out_shape=jax.ShapeDtypeStruct(x_blk.shape, bf),
        in_specs=[anyspec] * 6 + [vmspec],
        out_specs=anyspec,
        scratch_shapes=[
            vm(h.shape, bf), vm((CHUNKS, rows, k_dim, cw), bf), vm((SEND_SLOTS, chips) + piece, bf), vm((sends, chips) + piece, bf), vm((X_SLOTS, chips) + piece, bf),
            vm((units, 2) + piece, bf), vm((units, 2, patches, cw), bf), vm((3, CHUNKS) + piece, bf), vm((CHUNKS,) + piece, bf), vm((CHUNKS,) + piece, bf),
            vm((2, CHUNKS) + piece, bf),
            dma((5 * CHUNKS + rows,)), dma((CHUNKS, 2)), dma((CHUNKS, 2)), dma((CHUNKS,)), dma((CHUNKS,)), dma((CHUNKS, 2)), dma((CHUNKS, 2)), dma((CHUNKS,)), dma((CHUNKS,)),
            dma((units, 2)), dma((units, 2)), dma((units, 2)), dma((units, 2)), dma((sends, chips)), dma((sends, chips)), dma((CHUNKS,)), dma((CHUNKS,)),
            dma((CHUNKS,)), dma((CHUNKS,)), dma((2, CHUNKS, 4)), dma((2, CHUNKS, 4)), dma((2, CHUNKS, 4)), dma((2, CHUNKS, 4)), dma((2, CHUNKS)),
        ],
        compiler_params=pltpu.CompilerParams(collective_id=1, has_side_effects=True, vmem_limit_bytes=VMEM_MAX),
        cost_estimate=pl.CostEstimate(flops=2 * h.shape[0] * k_dim * dim_local * rows, bytes_accessed=1 << 27, transcendentals=0),
        name='stage_two',
    )(x_blk, h, w_o, w_down, w2_own, w2_cross, b_out.reshape(1, dim_local))


def copy_kernel(src, dst, held, in_sem, out_sem):
    count = in_sem.shape[0]
    step = src.shape[0] // count
    loads = [pltpu.make_async_copy(src.at[pl.ds(n * step, step)], held.at[pl.ds(n * step, step)], in_sem.at[n]) for n in range(count)]
    stores = [pltpu.make_async_copy(held.at[pl.ds(n * step, step)], dst.at[pl.ds(n * step, step)], out_sem.at[n]) for n in range(count)]
    for c in loads:
        c.start()
    for n in range(count):
        loads[n].wait()
        stores[n].start()
    for c in stores:
        c.wait()


def copy_out(array):
    count = 16
    return pl.pallas_call(
        copy_kernel,
        out_shape=jax.ShapeDtypeStruct(array.shape, array.dtype),
        in_specs=[pl.BlockSpec(memory_space=pl.ANY)],
        out_specs=pl.BlockSpec(memory_space=pl.ANY),
        scratch_shapes=[pltpu.VMEM(array.shape, array.dtype), pltpu.SemaphoreType.DMA((count,)), pltpu.SemaphoreType.DMA((count,))],
        compiler_params=pltpu.CompilerParams(vmem_limit_bytes=VMEM_MAX),
        name='copy_out',
    )(array)


def solution(mesh):
    rows, cols = mesh.shape['m1'], mesh.shape['m2']
    chips = cols // CORES
    assert rows == 4 and chips == 4

    def local_layer(x_blk, ln_scale, qn_scale, kn_scale, w_qkv, w_up, b_up, w_o, w_down, b_out):
        h, w2_own, w2_cross = stage_one(
            rows, chips, x_blk, ln_scale[None], qn_scale[None], kn_scale[None], b_up[None], w_qkv.transpose(1, 0, 2), w_up, w_o, w_down
        )
        return copy_out(stage_two(rows, chips, x_blk, h, w_o, w_down, w2_own, w2_cross, b_out))

    return jax.shard_map(local_layer, mesh=mesh, in_specs=(P('dp', None, 'm1'), P(), P(), P(), P('m1', None, 'm2'), P('m1', 'm2'), P('m2'), P('m2', 'm1'), P('m2', 'm1'), P('m1')), out_specs=P('dp', None, 'm1'), check_vma=False)
```

```python
import functools

import jax
import jax.numpy as jnp
from jax import lax
from jax.experimental import pallas as pl
from jax.experimental.pallas import tpu as pltpu
from jax.sharding import PartitionSpec as P

LN_EPS = 1e-6
CORES = 2
LINES = 16
LANES = 128
NEXT_CHUNK = (2, 3, 4, None, 5, 6, None)
CHUNKS = 4
X_SLOTS = 6
SEND_SLOTS = 3
PLAN = (
    ('send', 1, 2), ('part', 3, 2, 0), ('part', 2, 0, 1), ('mid', 0), ('mid', 1), ('part', 3, 0, 2), ('sum', 3, 2, 0), ('pass', 2, 3),
    ('send', 0, 2), ('pair', 1, 0, 3), ('sum', 2, 0, 1), ('mid', 2), ('part', 2, 2, 4), ('send', 2, 3), ('sum', 3, 0, 2), ('home', 0, 3),
    ('pair', 0, 0, 5), ('mid', 4), ('pass', 2, 1), ('home', 0, 0, 5), ('pass', 0, 3), ('send', 0, 3), ('pair', 2, 1, 6), ('pass', 1, 3),
    ('near', 0, 0), ('home', 0, 1, 3), ('pass', 3, 3), ('pass', 0, 1), ('sum', 2, 1, 6), ('sum', 2, 2, 4), ('send', 3, 3), ('near', 0, 3),
    ('pair', 0, 1, 7), ('pass', 3, 1), ('home', 0, 2), ('far', 0, 0), ('sum', 0, 1, 7), ('far', 0, 3), ('near', 0, 1), ('send', 1, 3),
    ('pass', 1, 1), ('near', 0, 2), ('pair', 3, 1, 8), ('home', 1, 0), ('far', 0, 1), ('sum', 3, 1, 8), ('far', 0, 2), ('home', 1, 2),
    ('pair', 1, 1, 9), ('near', 1, 2), ('near', 1, 0), ('sum', 1, 1, 9), ('home', 1, 3), ('home', 1, 1), ('near', 1, 3), ('near', 1, 1),
    ('far', 1, 3), ('far', 1, 0), ('far', 1, 2), ('far', 1, 1),
)
INNER_ORDER = ((2, 3), (1, 3), (0, 3), (2, 1), (3, 3), (0, 1), (3, 1), (1, 1))
VMEM_MAX = 67043328
MESH = pl.DeviceIdType.MESH


def layer_norm(values, scale):
    mean = jnp.mean(values, axis=-1, keepdims=True)
    centered = values - mean
    variance = jnp.mean(centered * centered, axis=-1, keepdims=True)
    return centered * lax.rsqrt(variance + LN_EPS) * scale


class Place:
    def __init__(self, rows, chips):
        self.rows, self.chips = rows, chips
        self.dp, self.row = lax.axis_index('dp'), lax.axis_index('m1')
        col = lax.axis_index('m2')
        self.col, self.chip, self.core = col, col // CORES, lax.rem(col, CORES)
        self.inner = self.row + 1 - 2 * lax.rem(self.row, 2)
        self.cross = rows - 1 - self.row
        self.pair = self.row // 2
        self.half = lax.rem((self.row + 1) // 2, 2)
        self.primary = self.core == self.pair
        self.inner_peer = (self.dp, self.inner, col)
        self.cross_peer = (self.dp, self.cross, col)
        self.right_peer = (self.dp, self.row, self.at(1) * CORES + self.core)
        self.left_peer = (self.dp, self.row, self.at(chips - 1) * CORES + self.core)
        self.sibling = (self.dp, self.row, self.chip * CORES + 1 - self.core)

    def at(self, dx):
        return lax.rem(self.chip + dx, self.chips)

    def enter(self):
        barrier = pltpu.get_barrier_semaphore()
        partners = (self.inner_peer, self.cross_peer, self.right_peer, self.left_peer, self.sibling)
        for who in partners:
            pl.semaphore_signal(barrier, inc=1, device_id=who, device_id_type=MESH)
        pl.semaphore_wait(barrier, len(partners))

    def first_image(self, half, dx, core, batch):
        per = batch // (2 * CORES)
        return (half * CORES + core) * per + self.at(dx) * (per // self.chips)


def remote(src, dst, ssem, rsem, who):
    return pltpu.make_async_remote_copy(src_ref=src, dst_ref=dst, send_sem=ssem, recv_sem=rsem, device_id=who, device_id_type=MESH)


def aligned(index, size):
    return pl.ds(pl.multiple_of(index * size, size), size)


def stage_one_kernel(rows, chips, heads, x_hbm, ln_all, qn_scale, kn_scale, bias_own, wq, wu, w_o, w_down, h_hbm, raw, w2_own, w2_cross, u_v, w_v, qkv_v, st_v, up_v, last_v, at_v, bias_v, ln_scale,
                     xs_send, xs_recv, ag_send, ag_recv, ld_sem, own_sem, b_send, b_recv, wa_send, wa_recv, wb_send, wb_recv, wc_send, wc_recv,
                     wd_send, wd_recv, up_sem, at_sem, v_send, v_recv, last_sem):
    p = Place(rows, chips)
    batch, patches, dim_local = x_hbm.shape
    dim = dim_local * rows
    wide = wq.shape[2]
    head_dim = wide // heads
    n_q, n_up = wq.shape[0], wu.shape[1] // wide
    n_w = n_q + n_up
    sub = batch // (2 * CORES * chips)
    group = sub * patches
    dx_of = (0, chips - 1, 1, 2)

    xa = remote(x_hbm.at[pl.ds(p.first_image(p.half, 0, p.core, batch), sub)], raw.at[0, 1], xs_send.at[0], xs_recv.at[0], p.cross_peer)
    xb = remote(x_hbm.at[pl.ds(p.first_image(1 - p.half, 0, p.core, batch), sub)], raw.at[0, 0], xs_send.at[1], xs_recv.at[1], p.inner_peer)
    xc = remote(raw.at[0, 0], raw.at[0, 2], xs_send.at[2], xs_recv.at[2], p.cross_peer)

    def ag(e, k):
        src, dst = ((raw.at[0, e], raw.at[1, e]), (raw.at[0, e], raw.at[2, e]), (raw.at[1, e, 0], raw.at[3, e, 0]), (raw.at[2, e, 1], raw.at[3, e, 1]))[k]
        return remote(src, dst, ag_send.at[e, k], ag_recv.at[e, k], p.right_peer if k % 2 == 0 else p.left_peer)

    def block(r, k):
        return w_v.at[pl.ds(r * dim_local, dim_local), aligned(k, wide)]

    def from_own(k, make, act):
        @pl.when(k < n_q)
        def _():
            act(make(wq.at[jnp.minimum(k, n_q - 1)]))

        @pl.when(k >= n_q)
        def _():
            act(make(wu.at[:, aligned(jnp.maximum(k - n_q, 0), wide)]))

    def wa(k, src=None):
        return remote(block(1, k) if src is None else src, block(1, k), wa_send.at[k], wa_recv.at[k], p.inner_peer)

    def wb(k, src=None):
        return remote(block(2, k) if src is None else src, block(2, k), wb_send.at[k], wb_recv.at[k], p.cross_peer)

    def wc(k):
        return remote(block(2, k), block(3, k), wc_send.at[k], wc_recv.at[k], p.inner_peer)

    def wd(r, k, src=None):
        return remote(block(r, k) if src is None else src, block(r, k), wd_send.at[r, k], wd_recv.at[r, k], p.sibling)

    own_copies = [pltpu.make_async_copy(wq.at[k], block(0, k), own_sem.at[k]) for k in range(n_q)]
    own_copies.append(pltpu.make_async_copy(wu, w_v.at[pl.ds(0, dim_local), pl.ds(n_q * wide, n_up * wide)], own_sem.at[n_q]))
    bias_copy = remote(bias_own, bias_v, b_send, b_recv, p.sibling)

    ko, kd = w_o.shape[0], w_down.shape[0]

    def two(dst, n, who):
        return [remote(w_o, dst.at[pl.ds(0, ko), :], v_send.at[n], v_recv.at[n], who), remote(w_down, dst.at[pl.ds(ko, kd), :], v_send.at[n + 1], v_recv.at[n + 1], who)]

    v_own, v_cross = two(w2_own, 0, p.sibling), two(w2_cross, 2, p.cross_peer)

    for r, source in enumerate((p.row, p.inner, p.cross, lax.rem(p.row + 2, rows))):
        ln_scale[:, r * dim_local : (r + 1) * dim_local] = ln_all[:, aligned(source, dim_local)]

    def start(copy):
        copy.start()

    def pump(k):
        @pl.when(p.primary)
        def _():
            wb(k).wait_recv()
            for c in wc_last if k == n_w - 1 else [wc(k)]:
                c.start()
            wd(2, k).start()
            later = NEXT_CHUNK[k]
            if later is not None:
                from_own(later, functools.partial(wa, later), start)
                from_own(later, functools.partial(wd, 0, later), start)

    def last_half(r, n):
        return w_v.at[pl.ds(r * dim_local, dim_local), pl.ds((n_w - 1) * wide + n * (wide // 2), wide // 2)]

    wc_last = [remote(last_half(2, n), last_half(3, n), wc_send.at[n_w - 1 + n], wc_recv.at[n_w - 1 + n], p.inner_peer) for n in range(2)]
    wd_last = [remote(last_half(3, n), last_half(3, n), wd_send.at[n, n_w], wd_recv.at[n, n_w], p.sibling) for n in range(2)]

    def hand_over(k):
        @pl.when(p.primary)
        def _():
            wa(k).wait_recv()
            wd(1, k).start()
            wc(k).wait_recv()
            wd(3, k).start()

    def receive(k):
        @pl.when(jnp.logical_not(p.primary))
        def _():
            for r in range(rows):
                wd(r, k).wait_recv()

    def load_copies(rank_dx, rank, s, b):
        image = p.first_image(p.half, rank_dx, p.core, batch) + s
        yield pltpu.make_async_copy(x_hbm.at[image], st_v.at[b, :, pl.ds(0, dim_local)], ld_sem.at[b, 0])
        for e in range(rows - 1):
            yield pltpu.make_async_copy(raw.at[rank, e, s], st_v.at[b, :, pl.ds((e + 1) * dim_local, dim_local)], ld_sem.at[b, e + 1])

    def normalize(ranks):
        jobs = [(rank, s) for rank in ranks for s in range(sub)]
        loads = [list(load_copies(dx_of[rank], rank, s, n % 2)) for n, (rank, s) in enumerate(jobs)]
        for n in range(len(jobs)):
            if n == 0:
                for c in loads[0]:
                    c.start()
            if n + 1 < len(jobs):
                for c in loads[n + 1]:
                    c.start()
            for c in loads[n]:
                c.wait()
            rank, s = jobs[n]

            def lines(m, carry, b=n % 2, base=(rank * sub + s) * patches):
                here = aligned(m, LINES)
                to = pl.ds(pl.multiple_of(base + m * LINES, LINES), LINES)
                parts = [slice(j * LANES, (j + 1) * LANES) for j in range(dim // LANES)]

                def load(part):
                    return st_v[b, here, part].astype(jnp.float32)

                mean = jnp.sum(functools.reduce(jnp.add, [load(part) for part in parts]), axis=-1, keepdims=True) / dim
                squares = [(load(part) - mean) * (load(part) - mean) for part in parts]
                inverse = lax.rsqrt(jnp.sum(functools.reduce(jnp.add, squares), axis=-1, keepdims=True) / dim + LN_EPS)
                for part in parts:
                    u_v[to, part] = ((load(part) - mean) * inverse * ln_scale[:, part]).astype(jnp.bfloat16)
                return carry

            lax.fori_loop(0, patches // LINES, lines, 0, unroll=4)

    def dot_cell(rank, k):
        return jnp.dot(u_v[aligned(rank, group), :], w_v[:, aligned(k, wide)], preferred_element_type=jnp.float32).astype(jnp.bfloat16)

    def qkv_cell(rank, k):
        z = dot_cell(rank, k)
        to = aligned(rank, group)

        @pl.when(k == n_q - 1)
        def _():
            qkv_v[k, to, :] = z

        @pl.when(k < n_q - 1)
        def _():
            scale = jnp.where(k == 0, qn_scale[...], kn_scale[...])
            for hd in range(heads):
                part = slice(hd * head_dim, (hd + 1) * head_dim)
                qkv_v[k, to, part] = layer_norm(z[:, part].astype(jnp.float32), scale).astype(jnp.bfloat16)

    def at_copy(image, b):
        return pltpu.make_async_copy(at_v.at[b], h_hbm.at[aligned(image, patches), pl.ds(0, wide)], at_sem.at[b])

    def attend(first, count):
        def one(image, carry):
            b = lax.rem(image, 2)
            here = aligned(image, patches)

            @pl.when(image >= 2)
            def _():
                at_copy(image - 2, b).wait()

            for hd in range(heads):
                part = slice(hd * head_dim, (hd + 1) * head_dim)
                q, k, v = (qkv_v[n, here, part] for n in range(3))
                scores = lax.dot_general(q, k, (((1,), (1,)), ((), ())), preferred_element_type=jnp.float32) * head_dim ** -0.5
                probs = jnp.exp(scores - jnp.max(scores, axis=-1, keepdims=True))
                probs = (probs / jnp.sum(probs, axis=-1, keepdims=True)).astype(jnp.bfloat16)
                at_v[b, :, part] = jnp.dot(probs, v, preferred_element_type=jnp.float32).astype(jnp.bfloat16)
            at_copy(image, b).start()
            return carry

        lax.fori_loop(first, first + count, one, 0)

    def up_copy(rank, k, b):
        return pltpu.make_async_copy(up_v.at[b], h_hbm.at[aligned(rank, group), aligned(k - n_q + 1, wide)], up_sem.at[b])

    def bias_of(here):
        return jnp.where(p.primary, bias_own[:, here], bias_v[:, here])

    def up_chunk(k, carry):
        hand_over(k)
        receive(k)
        bias = bias_of(aligned(k - n_q, wide))

        def cell(rank, carry):
            b = lax.rem(rank, 2)

            @pl.when(jnp.logical_or(k > n_q, rank >= 2))
            def _():
                up_copy(rank, k, b).wait()

            m = dot_cell(rank, k).astype(jnp.float32) + bias
            up_v[b] = (0.5 * m * (1.0 + lax.erf(m * 0.5 ** 0.5))).astype(jnp.bfloat16)
            up_copy(rank, k, b).start()
            return carry

        return lax.fori_loop(0, rows, cell, carry)

    def last_copy(rank, n):
        to = pl.ds(wide + (n_up - 1) * wide + n * (wide // 2), wide // 2)
        return pltpu.make_async_copy(last_v.at[n, lax.rem(rank, 2)], h_hbm.at[aligned(rank, group), to], last_sem.at[n, lax.rem(rank, 2)])

    def last_chunk(n):
        @pl.when(p.primary)
        def _():
            if n == 0:
                wa(n_w - 1).wait_recv()
                wd(1, n_w - 1).start()
            wc_last[n].wait_recv()
            wd_last[n].start()

        @pl.when(jnp.logical_not(p.primary))
        def _():
            if n == 0:
                for r in range(rows - 1):
                    wd(r, n_w - 1).wait_recv()
            wd_last[n].wait_recv()

        first = (n_up - 1) * wide + n * (wide // 2)
        bias = bias_of(pl.ds(first, wide // 2))
        weight = pl.ds(n_q * wide + first, wide // 2)

        def cell(rank, carry):
            @pl.when(rank >= 2)
            def _():
                last_copy(rank - 2, n).wait()

            m = jnp.dot(u_v[aligned(rank, group), :], w_v[:, weight], preferred_element_type=jnp.float32).astype(jnp.bfloat16).astype(jnp.float32) + bias
            last_v[n, lax.rem(rank, 2)] = (0.5 * m * (1.0 + lax.erf(m * 0.5 ** 0.5))).astype(jnp.bfloat16)
            last_copy(rank, n).start()
            return carry

        lax.fori_loop(0, rows, cell, 0)

    p.enter()
    xb.start()

    @pl.when(jnp.logical_not(p.primary))
    def _():
        from_own(0, functools.partial(wb, 0), start)

    xa.start()
    bias_copy.start()

    @pl.when(p.primary)
    def _():
        for c in own_copies:
            c.start()
        for k in range(NEXT_CHUNK[0]):
            from_own(k, functools.partial(wa, k), start)
            from_own(k, functools.partial(wd, 0, k), start)

    xb.wait_recv()
    xc.start()
    ag(0, 0).start()
    ag(0, 1).start()

    @pl.when(jnp.logical_not(p.primary))
    def _():
        for k in range(1, n_w):
            from_own(k, functools.partial(wb, k), start)
        for c in v_cross:
            c.start()

    pump(0)
    xa.wait_recv()
    ag(1, 0).start()
    ag(1, 1).start()
    xc.wait_recv()
    ag(2, 0).start()
    ag(2, 1).start()
    normalize((0,))

    def forward(e):
        for k in range(2):
            ag(e, k).wait_recv()
            ag(e, 2 + k).start()

    @pl.when(p.primary)
    def _():
        for c in own_copies:
            c.wait()
        for c in v_own:
            c.start()

    def cells(count, job):
        def cell(n, carry):
            qkv_cell(*job(n))
            return carry

        lax.fori_loop(0, count, cell, 0)

    forward(0)
    hand_over(0)
    pump(1)
    forward(1)
    receive(0)
    cells(1, lambda n: (n, n))
    hand_over(1)
    pump(2)
    receive(1)
    cells(1, lambda n: (n, n + 1))
    forward(2)
    normalize((1, 2))
    pump(3)
    cells((n_q - 1) * 2, lambda n: (1 + lax.rem(n, 2), n // 2))
    hand_over(2)
    receive(2)
    cells(rows - 1, lambda n: (n, n_q - 1))
    pump(4)
    attend(0, (rows - 1) * sub)
    pump(5)
    for e in range(rows - 1):
        ag(e, 2).wait_recv()
        ag(e, 3).wait_recv()
    normalize((rows - 1,))
    cells(n_q, lambda n: (rows - 1, n))
    pump(6)
    attend((rows - 1) * sub, sub)
    bias_copy.wait_recv()
    lax.fori_loop(n_q, n_w - 1, up_chunk, 0)
    last_chunk(0)
    last_chunk(1)

    for b in range(2):
        at_copy(b, b).wait()
        up_copy(b, n_q, b).wait()
        for n in range(2):
            last_copy(b, n).wait()
    for c in (xa, xb, xc, bias_copy):
        c.wait_send()
    for e in range(rows - 1):
        for k in range(4):
            ag(e, k).wait_send()

    @pl.when(p.primary)
    def _():
        for k in range(n_w):
            wa(k).wait_send()
            if k < n_w - 1:
                wc(k).wait_send()
            for r in range(rows if k < n_w - 1 else rows - 1):
                wd(r, k).wait_send()
        for c in v_own + wc_last + wd_last:
            c.wait_send()
        for c in v_cross:
            c.wait_recv()

    @pl.when(jnp.logical_not(p.primary))
    def _():
        for k in range(n_w):
            wb(k).wait_send()
        for c in v_cross:
            c.wait_send()
        for c in v_own:
            c.wait_recv()


def stage_one(rows, chips, x_blk, ln_scale, qn_scale, kn_scale, b_up, wq, wu, w_o, w_down):
    batch, patches, dim_local = x_blk.shape
    dim, wide = rows * dim_local, wq.shape[2]
    heads = wide // qn_scale.shape[1]
    n_q, n_up = wq.shape[0], wu.shape[1] // wide
    n_w = n_q + n_up
    sub = batch // (2 * CORES * chips)
    tokens = chips * sub * patches
    bf, vm, dma = jnp.bfloat16, pltpu.VMEM, pltpu.SemaphoreType.DMA
    anyspec, vmspec = pl.BlockSpec(memory_space=pl.ANY), pl.BlockSpec(memory_space=pltpu.VMEM)
    w2 = jax.ShapeDtypeStruct((w_o.shape[0] + w_down.shape[0], dim_local), bf)
    h, _, w2_own, w2_cross = pl.pallas_call(
        functools.partial(stage_one_kernel, rows, chips, heads),
        out_shape=(jax.ShapeDtypeStruct((tokens, wide + n_up * wide), bf), jax.ShapeDtypeStruct((chips, rows - 1, sub, patches, dim_local), bf), w2, w2),
        in_specs=[anyspec] + [vmspec] * 4 + [anyspec] * 4,
        out_specs=(anyspec,) * 4,
        scratch_shapes=[
            vm((tokens, dim), bf), vm((dim, n_w * wide), bf), vm((n_q, tokens, wide), bf), vm((2, patches, dim), bf),
            vm((2, sub * patches, wide), bf), vm((2, 2, sub * patches, wide // 2), bf), vm((2, patches, wide), bf), vm(b_up.shape, jnp.float32), vm(ln_scale.shape, jnp.float32),
            dma((3,)), dma((3,)), dma((rows - 1, 4)), dma((rows - 1, 4)), dma((2, rows)), dma((n_q + 1,)), dma, dma,
            dma((n_w,)), dma((n_w,)), dma((n_w,)), dma((n_w,)), dma((n_w + 1,)), dma((n_w + 1,)), dma((rows, n_w + 1)), dma((rows, n_w + 1)), dma((2,)), dma((2,)), dma((4,)), dma((4,)), dma((2, 2)),
        ],
        compiler_params=pltpu.CompilerParams(collective_id=0, has_side_effects=True, vmem_limit_bytes=VMEM_MAX),
        cost_estimate=pl.CostEstimate(flops=2 * tokens * dim * n_w * wide, bytes_accessed=1 << 27, transcendentals=0),
        name='stage_one',
    )(x_blk, ln_scale, qn_scale, kn_scale, b_up, wq, wu, w_o, w_down)
    return h, w2_own, w2_cross


def stage_two_kernel(rows, chips, x_hbm, h_hbm, w_o, w_down, w2_own, w2_cross, bias, out_hbm, h_v, w_v, ys_v, yt_v, x_v, rx_v, half_v, tot_v, t2_v, in_v, fin_v,
                     ld_sem, wa_send, wa_recv, wc_send, wc_recv, wd_send, wd_recv, wx_send, wx_recv, hf_send, hf_recv, x_send, x_recv, p_send, p_recv, t_send, t_recv,
                     i_send, i_recv, g_send, g_recv, s_send, s_recv, l_sem):
    p = Place(rows, chips)
    batch, patches, dim_local = x_hbm.shape
    sub = batch // (2 * CORES * chips)
    group = sub * patches
    ko, kd = w_o.shape[0], w_down.shape[0]
    cw = dim_local // CHUNKS
    far_rank = rows - 1
    sends = [step[1:] for step in PLAN if step[0] == 'send']
    units = [step for step in PLAN if step[0] in ('part', 'pair')]
    late = [step[1] for step in PLAN if step[0] == 'sum' and step[2] == 2]

    def cols(c):
        return pl.ds(c * cw, cw)

    def two(c, slot, make):
        return [make(w_o.at[:, cols(c)], w_v.at[c, slot, pl.ds(0, ko), :], 0), make(w_down.at[:, cols(c)], w_v.at[c, slot, pl.ds(ko, kd), :], 1)]

    wa = [two(c, 1, lambda s, d, n, c=c: remote(s, d, wa_send.at[c, n], wa_recv.at[c, n], p.inner_peer)) for c in range(CHUNKS)]
    wc = [remote(w2_cross.at[:, cols(c)], w_v.at[c, 3], wc_send.at[c], wc_recv.at[c], p.inner_peer) for c in range(CHUNKS)]
    wd = [{r: remote(w_v.at[c, r], w_v.at[c, r], wd_send.at[c, r // 2], wd_recv.at[c, r // 2], p.sibling) for r in (1, 3)} for c in range(CHUNKS)]
    wx = [remote(w2_cross.at[:, cols(c)], w_v.at[c, 2], wx_send.at[c], wx_recv.at[c], p.sibling) for c in range(CHUNKS)]
    own_primary = [two(c, 0, lambda s, d, n, c=c: pltpu.make_async_copy(s, d, ld_sem.at[2 * c + n])) for c in range(CHUNKS)]
    own_other = [pltpu.make_async_copy(w2_own.at[:, cols(c)], w_v.at[c, 0], ld_sem.at[2 * c]) for c in range(CHUNKS)]
    cross_load = [pltpu.make_async_copy(w2_cross.at[:, cols(c)], w_v.at[c, 2], ld_sem.at[2 * CHUNKS + c]) for c in range(CHUNKS)]
    def h_copy(rank):
        return pltpu.make_async_copy(h_hbm.at[aligned(rank, group), :], h_v.at[aligned(rank, group), :], ld_sem.at[5 * CHUNKS + rank])


    def images(side, dx):
        return p.first_image(p.half if side == 0 else 1 - p.half, dx, p.core, batch)

    fin_load = [
        [pltpu.make_async_copy(x_hbm.at[pl.ds(images(side, 0), sub), :, cols(c)], fin_v.at[side, c], ld_sem.at[3 * CHUNKS + side * CHUNKS + c]) for c in range(CHUNKS)]
        for side in (0, 1)
    ]

    def p_copy(n, rank):
        return remote(ys_v.at[n % SEND_SLOTS, rank], yt_v.at[n, rank], p_send.at[n, rank], p_recv.at[n, rank], p.cross_peer)

    def half_copy(u, k):
        who = p.right_peer if k == 0 else p.left_peer
        return remote(x_v.at[u % X_SLOTS, far_rank, k], half_v.at[u, k], hf_send.at[u, k], hf_recv.at[u, k], who)

    def x_copy(u, k):
        who = p.right_peer if k == 0 else p.left_peer
        return remote(x_v.at[u % X_SLOTS, 2 - k], rx_v.at[u, k], x_send.at[u, k], x_recv.at[u, k], who)

    def t_copy(c):
        return remote(tot_v.at[1, c], t2_v.at[c], t_send.at[c], t_recv.at[c], p.cross_peer)

    def i_copy(c):
        return remote(tot_v.at[2, c], in_v.at[c], i_send.at[c], i_recv.at[c], p.inner_peer)

    def spot(side, dx, c, count=sub, first=0):
        return out_hbm.at[pl.ds(images(side, dx) + first, count), :, cols(c)]

    def g_copy(side, c, k):
        who = p.right_peer if k % 2 == 0 else p.left_peer
        if k < 2:
            src, dst = fin_v.at[side, c], spot(side, 0, c)
        else:
            src = dst = spot(side, chips - 1 if k == 2 else 1, c, 1, k - 2)
        return remote(src, dst, g_send.at[side, c, k], g_recv.at[side, c, k], who)

    def s_copy(side, c, k):
        here = spot(side, (0, chips - 1, 1, 2)[k], c)
        return remote(fin_v.at[side, c] if k == 0 else here, here, s_send.at[side, c, k], s_recv.at[side, c, k], p.sibling)

    def l_copy(side, c):
        return pltpu.make_async_copy(fin_v.at[side, c], spot(side, 0, c), l_sem.at[side, c])

    def add(a, b):
        return a.astype(jnp.float32) + b.astype(jnp.float32)

    def dot(rank, c, r):
        return jnp.dot(h_v[aligned(rank, group), :], w_v[c, r], preferred_element_type=jnp.float32).astype(jnp.bfloat16).reshape(sub, patches, cw)

    def own_load(c, act):
        @pl.when(p.primary)
        def _():
            for copy in own_primary[c]:
                act(copy)

        @pl.when(jnp.logical_not(p.primary))
        def _():
            act(own_other[c])

    def received(c, r):
        if r == 0:
            own_load(c, lambda copy: copy.wait())
        elif r == 2:

            @pl.when(p.primary)
            def _():
                cross_load[c].wait()

            @pl.when(jnp.logical_not(p.primary))
            def _():
                wx[c].wait_recv()

        elif r:

            @pl.when(jnp.logical_not(p.primary))
            def _():
                wd[c][r].wait_recv()

    def cross_part(c, r):
        received(c, r)
        number = sends.index((c, r))
        if number >= SEND_SLOTS:
            for rank in range(chips):
                p_copy(number - SEND_SLOTS, rank).wait_send()

        def cell(n, carry):
            rank = far_rank - n
            if number == 0:
                h_copy(rank).wait()
            ys_v[number % SEND_SLOTS, rank] = dot(rank, c, r)
            p_copy(number, rank).start()
            return carry

        lax.fori_loop(0, chips, cell, 0)

    def reuse(u):
        if u >= X_SLOTS:
            for k in range(2):
                half_copy(u - X_SLOTS, k).wait_send()
                x_copy(u - X_SLOTS, k).wait_send()

    def mid_one(u, k):
        half_copy(u, k).wait_recv()
        s = u % X_SLOTS
        x_v[s, 2 - k, k] = add(x_v[s, 2 - k, k], half_v[u, k]).astype(jnp.bfloat16)
        x_copy(u, k).start()

    def pair_part(u, c, r):
        reuse(u)
        s = u % X_SLOTS
        received(c, r)
        number = sends.index((c, r + 2))

        def cell(n, carry):
            rank = far_rank - n
            part = dot(rank, c, r)
            p_copy(number, rank).wait_recv()
            x_v[s, rank] = add(part, yt_v[number, rank]).astype(jnp.bfloat16)

            @pl.when(n == 0)
            def _():
                half_copy(u, 0).start()
                half_copy(u, 1).start()

            for k in range(2):

                @pl.when(n == k + 1)
                def _(k=k):
                    mid_one(u, k)

            return carry

        lax.fori_loop(0, chips, cell, 0)

    def compute(u, c, r):
        reuse(u)
        s = u % X_SLOTS
        received(c, r)

        def cell(n, carry):
            rank = far_rank - n
            x_v[s, rank] = dot(rank, c, r)

            @pl.when(n == 0)
            def _():
                half_copy(u, 0).start()
                half_copy(u, 1).start()

            return carry

        lax.fori_loop(0, chips, cell, 0)

    def mid(u):
        mid_one(u, 0)
        mid_one(u, 1)

    def total(u, n):
        s = u % X_SLOTS
        return add(x_v[s, 0, n], rx_v[u, 0, n]) + rx_v[u, 1, n].astype(jnp.float32)

    def arrived(u):
        x_copy(u, 0).wait_recv()
        x_copy(u, 1).wait_recv()

    def reduce(u, c, slot, send=None):
        arrived(u)
        for n in range(sub):
            tot_v[slot, c, n] = total(u, n).astype(jnp.bfloat16)
        if send is not None:
            send(c).start()

    def fetch_far(c):
        @pl.when(p.primary)
        def _():
            wc[c].wait_recv()
            wd[c][3].start()

    def fetch_inner(c):
        @pl.when(p.primary)
        def _():
            for copy in wa[c]:
                copy.wait_recv()
            wd[c][1].start()

    def home(side, c, u=None):
        if u is None:
            (i_copy if side else t_copy)(c).wait_recv()
        else:
            arrived(u)
        fin_load[side][c].wait()
        for n in range(sub):
            if u is not None:
                summed = total(u, n)
            else:
                summed = in_v[c, n].astype(jnp.float32) if side else add(tot_v[0, c, n], t2_v[c, n])
            fin_v[side, c, n] = (fin_v[side, c, n].astype(jnp.float32) + summed + bias[:, cols(c)]).astype(jnp.bfloat16)
        g_copy(side, c, 0).start()
        g_copy(side, c, 1).start()
        s_copy(side, c, 0).start()
        l_copy(side, c).start()

    def near(side, c):
        for k in range(2):
            g_copy(side, c, k).wait_recv()
            g_copy(side, c, 2 + k).start()
            s_copy(side, c, 1 + k).start()

    def far(side, c):
        g_copy(side, c, 2).wait_recv()
        g_copy(side, c, 3).wait_recv()
        s_copy(side, c, 3).start()

    for rank in reversed(range(chips)):
        h_copy(rank).start()
    needs = [step[1:3] for step in PLAN if step[0] in ('send', 'part', 'pair')]
    for c, r in needs:
        if r == 0:
            own_load(c, lambda copy: copy.start())
        elif r == 2:

            @pl.when(p.primary)
            def _(c=c):
                cross_load[c].start()

    for side in (0, 1):
        for c in range(CHUNKS):
            fin_load[side][c].start()
    p.enter()

    @pl.when(p.primary)
    def _():
        for c, r in needs:
            if r == 2:
                wx[c].start()
        for c, r in INNER_ORDER:
            for copy in [wc[c]] if r == 3 else wa[c]:
                copy.start()

    assert PLAN[0][0] == 'send'
    for step, *of in PLAN:
        if step == 'send':
            cross_part(*of)
        elif step == 'part':
            compute(of[2], of[0], of[1])
        elif step == 'pair':
            pair_part(of[2], of[0], of[1])
        elif step == 'mid':
            mid(*of)
        elif step == 'sum':
            c, r, u = of
            reduce(u, c, {0: 0, 2: 1, 1: 2}[r], {0: None, 2: t_copy, 1: i_copy}[r])
        elif step == 'pass':
            (fetch_far if of[1] == 3 else fetch_inner)(of[0])
        elif step == 'home':
            home(*of)
        elif step == 'near':
            near(*of)
        else:
            far(*of)

    for c in range(CHUNKS):
        for side in (0, 1):
            for k in range(4):
                s_copy(side, c, k).wait_recv()
                s_copy(side, c, k).wait_send()
                g_copy(side, c, k).wait_send()
            l_copy(side, c).wait()
        if c in late:
            t_copy(c).wait_send()
        i_copy(c).wait_send()
    for number in range(len(sends) - SEND_SLOTS, len(sends)):
        for rank in range(chips):
            p_copy(number, rank).wait_send()
    for u in range(len(units) - X_SLOTS, len(units)):
        for k in range(2):
            half_copy(u, k).wait_send()
            x_copy(u, k).wait_send()

    @pl.when(p.primary)
    def _():
        for c in range(CHUNKS):
            wc[c].wait_send()
            wx[c].wait_send()
            for copy in wa[c]:
                copy.wait_send()
            for r in (1, 3):
                wd[c][r].wait_send()


def stage_two(rows, chips, x_blk, h, w_o, w_down, w2_own, w2_cross, b_out):
    batch, patches, dim_local = x_blk.shape
    sub = batch // (2 * CORES * chips)
    k_dim, cw = w2_own.shape[0], dim_local // CHUNKS
    units = sum(step[0] in ('part', 'pair') for step in PLAN)
    sends = sum(step[0] == 'send' for step in PLAN)
    bf, vm, dma = jnp.bfloat16, pltpu.VMEM, pltpu.SemaphoreType.DMA
    piece = (sub, patches, cw)
    anyspec, vmspec = pl.BlockSpec(memory_space=pl.ANY), pl.BlockSpec(memory_space=pltpu.VMEM)
    return pl.pallas_call(
        functools.partial(stage_two_kernel, rows, chips),
        out_shape=jax.ShapeDtypeStruct(x_blk.shape, bf),
        in_specs=[anyspec] * 6 + [vmspec],
        out_specs=anyspec,
        scratch_shapes=[
            vm(h.shape, bf), vm((CHUNKS, rows, k_dim, cw), bf), vm((SEND_SLOTS, chips) + piece, bf), vm((sends, chips) + piece, bf), vm((X_SLOTS, chips) + piece, bf),
            vm((units, 2) + piece, bf), vm((units, 2, patches, cw), bf), vm((3, CHUNKS) + piece, bf), vm((CHUNKS,) + piece, bf), vm((CHUNKS,) + piece, bf),
            vm((2, CHUNKS) + piece, bf),
            dma((5 * CHUNKS + rows,)), dma((CHUNKS, 2)), dma((CHUNKS, 2)), dma((CHUNKS,)), dma((CHUNKS,)), dma((CHUNKS, 2)), dma((CHUNKS, 2)), dma((CHUNKS,)), dma((CHUNKS,)),
            dma((units, 2)), dma((units, 2)), dma((units, 2)), dma((units, 2)), dma((sends, chips)), dma((sends, chips)), dma((CHUNKS,)), dma((CHUNKS,)),
            dma((CHUNKS,)), dma((CHUNKS,)), dma((2, CHUNKS, 4)), dma((2, CHUNKS, 4)), dma((2, CHUNKS, 4)), dma((2, CHUNKS, 4)), dma((2, CHUNKS)),
        ],
        compiler_params=pltpu.CompilerParams(collective_id=1, has_side_effects=True, vmem_limit_bytes=VMEM_MAX),
        cost_estimate=pl.CostEstimate(flops=2 * h.shape[0] * k_dim * dim_local * rows, bytes_accessed=1 << 27, transcendentals=0),
        name='stage_two',
    )(x_blk, h, w_o, w_down, w2_own, w2_cross, b_out.reshape(1, dim_local))


def copy_kernel(src, dst, held, in_sem, out_sem):
    count = in_sem.shape[0]
    step = src.shape[0] // count
    loads = [pltpu.make_async_copy(src.at[pl.ds(n * step, step)], held.at[pl.ds(n * step, step)], in_sem.at[n]) for n in range(count)]
    stores = [pltpu.make_async_copy(held.at[pl.ds(n * step, step)], dst.at[pl.ds(n * step, step)], out_sem.at[n]) for n in range(count)]
    for c in loads:
        c.start()
    for n in range(count):
        loads[n].wait()
        stores[n].start()
    for c in stores:
        c.wait()


def copy_out(array):
    count = 16
    return pl.pallas_call(
        copy_kernel,
        out_shape=jax.ShapeDtypeStruct(array.shape, array.dtype),
        in_specs=[pl.BlockSpec(memory_space=pl.ANY)],
        out_specs=pl.BlockSpec(memory_space=pl.ANY),
        scratch_shapes=[pltpu.VMEM(array.shape, array.dtype), pltpu.SemaphoreType.DMA((count,)), pltpu.SemaphoreType.DMA((count,))],
        compiler_params=pltpu.CompilerParams(vmem_limit_bytes=VMEM_MAX),
        name='copy_out',
    )(array)


def solution(mesh):
    rows, cols = mesh.shape['m1'], mesh.shape['m2']
    chips = cols // CORES
    assert rows == 4 and chips == 4

    def local_layer(x_blk, ln_scale, qn_scale, kn_scale, w_qkv, w_up, b_up, w_o, w_down, b_out):
        h, w2_own, w2_cross = stage_one(
            rows, chips, x_blk, ln_scale[None], qn_scale[None], kn_scale[None], b_up[None], w_qkv.transpose(1, 0, 2), w_up, w_o, w_down
        )
        return copy_out(stage_two(rows, chips, x_blk, h, w_o, w_down, w2_own, w2_cross, b_out))

    return jax.shard_map(local_layer, mesh=mesh, in_specs=(P('dp', None, 'm1'), P(), P(), P(), P('m1', None, 'm2'), P('m1', 'm2'), P('m2'), P('m2', 'm1'), P('m2', 'm1'), P('m1')), out_specs=P('dp', None, 'm1'), check_vma=False)
```
